128 devices in a mesh: band: 32 (over y, x, core), sub: 4 (over z).
Axes of the slice: x: 4, y: 4, z: 4, core: 2. Of those that a mesh axis runs over, the one named last changes fastest.
Arguments:
- fields: bfloat16 [12, 4194304], P(None, ('band', 'sub')), may hold values from -1.5 to 6
- land_mask: int32 [4194304], P(('band', 'sub')), may hold values from 0 to 1
- intersection: bfloat16 [32768, 128, 128], P(('band', 'sub')), as said below
- send_slot: int32 [32768], P(('band', 'sub')), may hold values from 0 to 511, as said below
- target_block: int32 [32768], P(('band', 'sub')), may hold values from 0 to 15
- live_blocks: int32 [128], P(('band', 'sub')), may hold values from 192 to 256, as said below
Outputs:
- remapped: float32 [12, 262144], P(None, ('band', 'sub'))
The draws below stay inside these ranges and needn't reach their ends.
Inputs may be any that keep to these rules, and one draw needn't show every extreme that they name: `send_slot`: within one device's 256 entries the values are distinct; value // 4 is the device that owns the block's target; in each device's entries some owner is named exactly 4 times and none more. `live_blocks`: some device has all 256 slots live in every draw. `intersection`: entries are positive.
All inputs are finite; a program needn't handle non-finite values.
Results may differ from the reference program's by a relative error of at most 0.0003.
Values may be sent and summed in bfloat16 or wider, within the bound.
A program may use at most 64 MiB of HBM per device.

```python
import jax
import jax.numpy as jnp
from jax import lax

F = 12
CELL = 128
SB_DEV = 256
TB_DEV = 16
CAP = 4
SB = 32768
TB = 2048
DEVICES = 128


def draw_intersection(key, part):
    first_key, second_key = jax.random.split(jax.random.fold_in(key, 11), 2)
    logs = jax.random.uniform(first_key, (SB, CELL, CELL), jnp.float32, jnp.log(0.001), jnp.log(0.02))
    offdiag = jnp.exp(logs)
    diagonal = jax.random.uniform(second_key, (SB, CELL), jnp.float32, 0.15, 0.35)
    weights = offdiag + jnp.eye(CELL, dtype=jnp.float32)[None, :, :] * diagonal[:, :, None]
    return weights.astype(jnp.bfloat16)


def draw_send_slot(key, part):
    base_key = jax.random.fold_in(key, 23)

    def device_slots(device):
        random_device_key = jax.random.fold_in(base_key, device)
        first_key, second_key, third_key = jax.random.split(random_device_key, 3)
        positions = DEVICES * CAP
        scores = jax.random.permutation(first_key, positions).astype(jnp.int32)
        chosen_owner = jax.random.randint(second_key, (), 0, DEVICES)
        places = jnp.arange(positions, dtype=jnp.int32)
        scores = jnp.where(places // CAP == chosen_owner, positions + places, scores)
        top_values, top_places = lax.top_k(scores, SB_DEV)
        ordering = jax.random.permutation(third_key, SB_DEV)
        return top_places[ordering].astype(jnp.int32)
    return jax.vmap(device_slots)(jnp.arange(DEVICES, dtype=jnp.int32)).reshape(-1)


def target_numbers(key):
    return jax.random.randint(jax.random.fold_in(key, 41), (SB,), 0, TB_DEV).astype(jnp.int32)


def draw_target_block(key, part):
    return target_numbers(key)


def draw_land_mask(key, part):
    slots = draw_send_slot(key, part)
    global_target = slots // CAP * TB_DEV + target_numbers(key)
    kinds = jax.random.randint(jax.random.fold_in(key, 43), (TB,), 0, 16).astype(jnp.int32)
    block_kind = kinds[global_target]
    first_key, second_key = jax.random.split(jax.random.fold_in(key, 47))
    block_draw = jax.random.randint(first_key, (SB,), 0, 16).astype(jnp.int32)
    cell_draw = jax.random.randint(second_key, (SB, CELL), 0, 16).astype(jnp.int32)
    coastal = (block_kind >= 1) & (block_kind < 4)
    inland = block_kind >= 4
    coastal_land = (coastal & (block_draw < 2))[:, None] & (cell_draw < 4)
    inland_land = (inland & (block_draw >= 5))[:, None] & (cell_draw < 13)
    land = (coastal_land | inland_land).astype(jnp.int32)
    return land.reshape(SB * CELL)


def draw_fields(key, part):
    first_key = jax.random.fold_in(jax.random.fold_in(key, 53), 0)
    device = (jnp.arange(SB * CELL, dtype=jnp.int32) // (SB_DEV * CELL)).astype(jnp.float32)
    position = device / max(DEVICES - 1, 1)
    level = (0.5 + 2.0 * position)[None, :]
    noise = jax.random.uniform(first_key, (F, SB * CELL), jnp.float32, -1.0, 1.0)
    return (level + noise).astype(jnp.bfloat16)


def draw_live_blocks(key, part):
    first_key, second_key = jax.random.split(jax.random.fold_in(key, 37))
    counts = jax.random.randint(first_key, (DEVICES,), 3 * SB_DEV // 4, SB_DEV + 1)
    full_device = jax.random.randint(second_key, (), 0, DEVICES)
    counts = jnp.where(jnp.arange(DEVICES) == full_device, SB_DEV, counts)
    return counts.astype(jnp.int32)


def setup_inputs(seed: int = 0) -> dict:
    streams_of = jax.random.split(jax.random.key(seed), 7)
    fields = draw_fields(jax.random.fold_in(streams_of[6], 71), 0)
    land_mask = draw_land_mask(jax.random.fold_in(streams_of[6], 71), 0)
    intersection = draw_intersection(jax.random.fold_in(streams_of[6], 71), 0)
    send_slot = draw_send_slot(jax.random.fold_in(streams_of[6], 71), 0)
    target_block = draw_target_block(jax.random.fold_in(streams_of[6], 71), 0)
    live_blocks = draw_live_blocks(jax.random.fold_in(streams_of[6], 71), 0)
    return dict(fields=fields, land_mask=land_mask, intersection=intersection, send_slot=send_slot, target_block=target_block, live_blocks=live_blocks)


def reference(fields, land_mask, intersection, send_slot, target_block, live_blocks):
    field_blocks = fields.reshape(F, DEVICES, SB_DEV, CELL).transpose(1, 2, 0, 3)
    mask_blocks = land_mask.reshape(DEVICES, SB_DEV, CELL)
    live_rows = (jnp.arange(SB_DEV, dtype=jnp.int32)[None, :] < live_blocks[:, None]).astype(jnp.int32)
    kept_mask = mask_blocks * live_rows[:, :, None]
    kept_float = kept_mask.astype(jnp.float32)
    masked = field_blocks * kept_mask[:, :, None, :].astype(jnp.bfloat16)
    totals = jnp.sum(masked.astype(jnp.float32), axis=(0, 1, 3))
    land_count = jnp.sum(kept_float)
    land_mean = totals / jnp.maximum(land_count, 1.0)
    stacked_fields = jnp.concatenate([masked, kept_mask[:, :, None, :].astype(jnp.bfloat16)], axis=2)
    weights = intersection.reshape(DEVICES, SB_DEV, CELL, CELL)
    global_target = ((send_slot.reshape(DEVICES, SB_DEV) // CAP) * TB_DEV + target_block.reshape(DEVICES, SB_DEV)).astype(jnp.int32)

    def add_device(accumulated, items):
        field_stack_part, remap_weight_part, target_part = items
        contribution_partial = jnp.einsum("myr,mrw->myw", field_stack_part.astype(jnp.float32), remap_weight_part.astype(jnp.float32))
        return accumulated.at[target_part].add(contribution_partial), None

    start_sums = jnp.zeros((TB_DEV * DEVICES, F + 1, CELL), jnp.float32)
    sums, unused = lax.scan(add_device, start_sums, (stacked_fields, weights, global_target))
    numer = sums[:, :F, :]
    fraction = sums[:, F, :]
    filled = numer + jnp.maximum(0.25 - fraction, 0.0)[:, None, :] * land_mean[None, :, None]
    remap_output = filled / jnp.maximum(fraction, 0.25)[:, None, :]
    return remap_output.transpose(1, 0, 2).reshape(F, TB_DEV * DEVICES * CELL)
```

```python
import functools

import jax
import jax.numpy as jnp
from jax import lax
from jax.experimental import pallas as pl
from jax.experimental.pallas import tpu as pltpu
from jax.sharding import PartitionSpec as P

CELL = 128
BLOCKS = 256
STEP = 32
TARGETS = 16
CHUNK = 64
ROWS = (4, 4, 5)
FIRST = (0, 4, 8)
ORDER = ("zxy", "xyz", "yzx")
MESH = pl.DeviceIdType.MESH


def local_kernel(
    pos_ref, target_ref, live_ref, fields_ref, mask_ref, weights_ref,
    out_a, out_b, out_c, codes_ref, total_ref, code_a, code_b, code_c,
):
    step = pl.program_id(0)
    outs = (out_a, out_b, out_c)
    codes = (code_a, code_b, code_c)

    @pl.when(step == 0)
    def _():
        total_ref[...] = jnp.zeros_like(total_ref)
        for ref in outs + codes:
            rows = ref.shape[0] // 8

            @pl.loop(0, rows // 8)
            def _(i):
                ref[pl.ds(pl.multiple_of(i * 64, 64), 64), :] = jnp.zeros((64, CELL), ref.dtype)

    total = total_ref[...]
    for block in range(STEP):
        index = step * STEP + block
        live = (index < live_ref[0]).astype(jnp.int32)
        mask = (mask_ref[pl.ds(block, 1), :] * live).astype(jnp.float32)
        values = fields_ref[:, block * CELL : (block + 1) * CELL].astype(jnp.float32)
        stacked = jnp.concatenate([values * mask, jnp.broadcast_to(mask, (4, CELL))], axis=0)
        total += stacked
        contrib = jnp.dot(
            stacked.astype(jnp.bfloat16), weights_ref[block], preferred_element_type=jnp.float32
        )
        target = target_ref[index]
        for g in range(3):
            pos = pos_ref[g, index]
            part = pos // CHUNK
            inner = pos - part * CHUNK
            base = part * (ROWS[g] * CHUNK) + inner
            outs[g][pl.ds(base, ROWS[g], stride=CHUNK), :] = contrib[FIRST[g] : FIRST[g] + ROWS[g]]
            code = (inner // 4) * TARGETS + target
            codes[g][pl.ds(pos, 1), :] = jnp.full((1, CELL), code.astype(jnp.float32))
    total_ref[...] = total

    @pl.when(step == BLOCKS // STEP - 1)
    def _():
        low = lax.broadcasted_iota(jnp.int32, (8, CELL), 1) < CHUNK
        for g in range(3):
            for pair in range(4):
                turned = codes[g][pl.ds(pair * CELL, CELL), :].T[0:8]
                rolled = pltpu.roll(turned, CHUNK, 1)
                even = jnp.where(low, turned, rolled).astype(jnp.int32)
                odd = jnp.where(low, rolled, turned).astype(jnp.int32)
                codes_ref[g, 2 * pair] = even
                codes_ref[g, 2 * pair + 1] = odd


def exchange_kernel(
    in_a, in_b, in_c, codes_ref, total_ref, out_ref,
    r1_a, r1_b, r1_c, c1, s2_a, s2_b, s2_c, r2_a, r2_b, r2_c,
    s3_a, s3_b, s3_c, r3_a, r3_b, r3_c, final_ref,
    t_send, t1, t2, t3,
    send1, recv1, csend, crecv, own1, send2, recv2, send3, recv3, tsend, trecv,
):
    ins = (in_a, in_b, in_c)
    r1 = (r1_a, r1_b, r1_c)
    s2 = (s2_a, s2_b, s2_c)
    r2 = (r2_a, r2_b, r2_c)
    s3 = (s3_a, s3_b, s3_c)
    r3 = (r3_a, r3_b, r3_c)
    band = lax.axis_index("band")
    here = {
        "y": band // 8,
        "x": lax.rem(band // 2, 4),
        "c": lax.rem(band, 2),
        "z": lax.axis_index("sub"),
    }

    def peer(dim, shift, core=0):
        at = dict(here)
        at[dim] = lax.rem(here[dim] + shift, 4)
        at["c"] = lax.rem(here["c"] + core, 2)
        return at, ((at["y"] * 4 + at["x"]) * 2 + at["c"], at["z"])

    def remote(src, dst, send, recv, device):
        return pltpu.make_async_remote_copy(
            src_ref=src, dst_ref=dst, send_sem=send, recv_sem=recv,
            device_id=device, device_id_type=MESH,
        )

    barrier = pltpu.get_barrier_semaphore()
    count = 0
    for dim in "zxy":
        for shift in (1, 2, 3):
            for core in (0, 1):
                pl.semaphore_signal(
                    barrier, inc=1, device_id=peer(dim, shift, core)[1], device_id_type=MESH
                )
                count += 1
    pl.semaphore_signal(barrier, inc=1, device_id=peer("z", 0, 1)[1], device_id_type=MESH)
    pl.semaphore_wait(barrier, count + 1)

    sends = []
    first = [[None] * 8 for _ in range(3)]
    first_codes = [[None] * 8 for _ in range(3)]
    totals_first = []
    local = []
    for shift, core in ((2, 0), (2, 1), (1, 0), (3, 0), (1, 1), (3, 1), (0, 1)):
        for g in range(3):
            dim = ORDER[g][0]
            at, device = peer(dim, shift, core)
            slot = shift * 2 + core
            code = remote(
                codes_ref.at[g, at["c"] * 4 + at[dim]], c1.at[g, slot],
                csend.at[g, slot], crecv.at[g, slot], device,
            )
            code.start()
            copy = remote(
                ins[g].at[at["c"] * 4 + at[dim]], r1[g].at[slot],
                send1.at[g, slot], recv1.at[g, slot], device,
            )
            copy.start()
            sends += [code, copy]
            first[g][slot] = copy
            first_codes[g][slot] = code
            if g == 0:
                whole = remote(total_ref, t1.at[slot], tsend.at[0, slot], trecv.at[0, slot], device)
                whole.start()
                sends.append(whole)
                totals_first.append((slot, whole))
    for g in range(3):
        mine = here["c"] * 4 + here[ORDER[g][0]]
        copy = pltpu.make_async_copy(ins[g].at[mine], r1[g].at[0], own1.at[g])
        copy.start()
        local.append(copy)
    total = total_ref[...]
    for slot, copy in totals_first:
        copy.wait_recv()
        total += t1[slot]
    t_send[0] = total
    totals_second = []
    for shift in (1, 2, 3):
        copy = remote(
            t_send.at[0], t2.at[shift - 1], tsend.at[1, shift], trecv.at[1, shift],
            peer("x", shift)[1],
        )
        copy.start()
        sends.append(copy)
        totals_second.append(copy)

    second = []
    for g in range(3):
        mine = here["c"] * 4 + here[ORDER[g][0]]
        low = lax.broadcasted_iota(jnp.int32, (1, CELL), 1) < CHUNK
        lanes = []
        for pair in range(4):
            if pair == 0:
                left = codes_ref[g, mine]
            else:
                first_codes[g][2 * pair].wait_recv()
                left = c1[g, 2 * pair]
            first_codes[g][2 * pair + 1].wait_recv()
            right = c1[g, 2 * pair + 1]
            lanes.append(jnp.where(low, left[0:1], right[0:1]))
        wide = jnp.concatenate(lanes, axis=1)
        rows = lax.broadcasted_iota(jnp.int32, (256, 512), 0)
        select = jnp.where(rows == wide, 1.0, 0.0).astype(jnp.bfloat16)
        local[g].wait()
        for slot in range(1, 8):
            first[g][slot].wait_recv()
        for row in range(ROWS[g]):
            data = jnp.concatenate([r1[g][slot, row] for slot in range(8)], axis=0)
            high = data.astype(jnp.bfloat16)
            rest = (data - high.astype(jnp.float32)).astype(jnp.bfloat16)
            both = jnp.dot(
                select, jnp.concatenate([high, rest], axis=1), preferred_element_type=jnp.float32
            )
            summed = both[:, :CELL] + both[:, CELL:]
            for part in range(4):
                s2[g][part, row] = summed[part * 64 : (part + 1) * 64]
        dim = ORDER[g][1]
        copies = []
        for shift in (2, 1, 3):
            at, device = peer(dim, shift)
            copy = remote(
                s2[g].at[at[dim]], r2[g].at[shift - 1], send2.at[g, shift], recv2.at[g, shift], device
            )
            copy.start()
            sends.append(copy)
            copies.append(copy)
        second.append(copies)

    total = t_send[0]
    for shift in (1, 2, 3):
        totals_second[shift - 1].wait_recv()
        total += t2[shift - 1]
    t_send[1] = total
    totals_third = []
    for shift in (1, 2, 3):
        copy = remote(
            t_send.at[1], t3.at[shift - 1], tsend.at[2, shift], trecv.at[2, shift],
            peer("y", shift)[1],
        )
        copy.start()
        sends.append(copy)
        totals_third.append(copy)

    third = []
    for g in range(3):
        for copy in second[g]:
            copy.wait_recv()
        mine = here[ORDER[g][1]]
        for row in range(ROWS[g]):
            summed = s2[g][mine, row] + r2[g][0, row] + r2[g][1, row] + r2[g][2, row]
            for part in range(4):
                s3[g][part, row] = summed[part * TARGETS : (part + 1) * TARGETS]
        dim = ORDER[g][2]
        copies = []
        for shift in (2, 1, 3):
            at, device = peer(dim, shift)
            copy = remote(
                s3[g].at[at[dim]], r3[g].at[shift - 1], send3.at[g, shift], recv3.at[g, shift], device
            )
            copy.start()
            sends.append(copy)
            copies.append(copy)
        third.append(copies)

    total = t_send[1]
    for shift in (1, 2, 3):
        totals_third[shift - 1].wait_recv()
        total += t3[shift - 1]
    total = jnp.sum(total, axis=1, keepdims=True)
    mean = total[0:12] / jnp.maximum(total[12:13], 1.0)
    for g in range(3):
        for copy in third[g]:
            copy.wait_recv()
        mine = here[ORDER[g][2]]
        for row in range(ROWS[g]):
            summed = s3[g][mine, row] + r3[g][0, row] + r3[g][1, row] + r3[g][2, row]
            final_ref[pl.ds((FIRST[g] + row) * TARGETS, TARGETS), :] = summed
    for t in range(TARGETS):
        numer = final_ref[pl.ds(t, 12, stride=TARGETS), :]
        fraction = final_ref[pl.ds(12 * TARGETS + t, 1), :]
        filled = numer + jnp.maximum(0.25 - fraction, 0.0) * mean
        out_ref[:, t * CELL : (t + 1) * CELL] = filled / jnp.maximum(fraction, 0.25)
    for copy in sends:
        copy.wait_send()


def body(fields, land_mask, intersection, send_slot, target_block, live_blocks):
    k = send_slot % 4
    owner = send_slot // 4
    z = owner % 4
    c = (owner // 4) % 2
    x = (owner // 8) % 4
    y = owner // 32
    at = {"x": x, "y": y, "z": z}
    pos = jnp.stack(
        [
            ((((c * 4 + at[o[0]]) * 4 + at[o[1]]) * 4 + at[o[2]]) * 4 + k).astype(jnp.int32)
            for o in ORDER
        ]
    )
    smem = pl.BlockSpec(memory_space=pltpu.SMEM)
    f32 = jnp.float32
    sizes = [8 * r * CHUNK for r in ROWS]
    whole = lambda shape: pl.BlockSpec(shape, lambda i: (0,) * len(shape))
    *parts, codes, total = pl.pallas_call(
        local_kernel,
        grid=(BLOCKS // STEP,),
        in_specs=[
            smem, smem, smem,
            pl.BlockSpec((12, STEP * CELL), lambda i: (0, i)),
            pl.BlockSpec((STEP, CELL), lambda i: (i, 0)),
            pl.BlockSpec((STEP, CELL, CELL), lambda i: (i, 0, 0)),
        ],
        out_specs=[whole((n, CELL)) for n in sizes] + [whole((3, 8, 8, CELL)), whole((16, CELL))],
        out_shape=[jax.ShapeDtypeStruct((n, CELL), f32) for n in sizes]
        + [jax.ShapeDtypeStruct((3, 8, 8, CELL), jnp.int32), jax.ShapeDtypeStruct((16, CELL), f32)],
        scratch_shapes=[pltpu.VMEM((512, CELL), f32)] * 3,
        compiler_params=pltpu.CompilerParams(dimension_semantics=("arbitrary",)),
        name="local",
    )(pos, target_block, live_blocks, fields, land_mask.reshape(BLOCKS, CELL), intersection)
    parts = [p.reshape(8, r, CHUNK, CELL) for p, r in zip(parts, ROWS)]
    vmem = pl.BlockSpec(memory_space=pltpu.VMEM)
    hbm = pl.BlockSpec(memory_space=pl.ANY)
    dma = pltpu.SemaphoreType.DMA
    return pl.pallas_call(
        exchange_kernel,
        in_specs=[hbm, hbm, hbm, vmem, vmem],
        out_specs=vmem,
        out_shape=jax.ShapeDtypeStruct((12, TARGETS * CELL), f32),
        scratch_shapes=[pltpu.VMEM((8, r, CHUNK, CELL), f32) for r in ROWS]
        + [pltpu.VMEM((3, 8, 8, CELL), jnp.int32)]
        + [pltpu.VMEM((4, r, CHUNK, CELL), f32) for r in ROWS]
        + [pltpu.VMEM((3, r, CHUNK, CELL), f32) for r in ROWS]
        + [pltpu.VMEM((4, r, TARGETS, CELL), f32) for r in ROWS]
        + [pltpu.VMEM((3, r, TARGETS, CELL), f32) for r in ROWS]
        + [pltpu.VMEM((13 * TARGETS, CELL), f32)]
        + [pltpu.VMEM((2, 16, CELL), f32), pltpu.VMEM((8, 16, CELL), f32)]
        + [pltpu.VMEM((3, 16, CELL), f32), pltpu.VMEM((3, 16, CELL), f32)]
        + [dma((3, 8)), dma((3, 8)), dma((3, 8)), dma((3, 8)), dma((3,))]
        + [dma((3, 4)), dma((3, 4)), dma((3, 4)), dma((3, 4)), dma((3, 8)), dma((3, 8))],
        compiler_params=pltpu.CompilerParams(collective_id=0, has_side_effects=True),
        name="exchange",
    )(*parts, codes, total)


def solution(mesh):
    axes = ("band", "sub")
    return jax.shard_map(
        body,
        mesh=mesh,
        in_specs=(P(None, axes), P(axes), P(axes, None, None), P(axes), P(axes), P(axes)),
        out_specs=P(None, axes),
        check_vma=False,
    )
```

```python
import jax
import jax.numpy as jnp
from jax import lax
from jax.experimental import pallas as pl
from jax.experimental.pallas import tpu as pltpu
from jax.sharding import PartitionSpec as P

CELL = 128
BLOCKS = 256
TARGETS = 16
CHUNK = 64
ROWS = (4, 4, 5)
FIRST = (0, 4, 8)
STAGES = ("zxy", "xyz", "yzx")
SLOTS = ("zxy", "xzy", "yzx")
MESH = pl.DeviceIdType.MESH
F32 = jnp.float32
BF16 = jnp.bfloat16
WEIGHT_COPIES = 4


def encode(tiles, lane, write):
    top = jnp.abs(tiles[0])
    for tile in tiles[1:]:
        top = jnp.maximum(top, jnp.abs(tile))
    top = jnp.maximum(jnp.max(top, axis=1, keepdims=True), 1e-25)
    power = jnp.ceil(jnp.log2(top) + 0.02)
    down = jnp.exp2(-power)
    for row, tile in enumerate(tiles):
        small = tile * down
        code = small * lax.rsqrt(jnp.abs(small) + 1e-30) * 32768.0
        write(row, jnp.round(code).astype(jnp.int32).astype(jnp.int16))
    scale = jnp.exp2(power - 30.0)
    lanes = lax.broadcasted_iota(jnp.int32, (16, CELL), 1) % CHUNK
    slots = lax.broadcasted_iota(jnp.int32, (16, CELL), 0) + lane
    return jnp.sum(jnp.where(lanes == slots, scale, 0.0), axis=0, keepdims=True)


def decode(codes):
    value = codes.astype(F32)
    value = value * jnp.abs(value)
    high = value.astype(BF16)
    return jnp.concatenate([high, (value - high.astype(F32)).astype(BF16)], axis=1)


def kernel(
    live_ref, slot_hbm, target_hbm, fields_hbm, mask_hbm, weights_hbm, out_ref,
    slot_ref, target_ref, fields_ref, mask_ref, weights_ref, stack_ref, index_vmem, index_smem,
    st_a, st_b, st_c, q_a, q_b, q_c, r1_a, r1_b, r1_c, cs, c1,
    s2_a, s2_b, s2_c, q2_a, q2_b, q2_c, r2_a, r2_b, r2_c, cs2, c2,
    s3_a, s3_b, s3_c, r3_a, r3_b, r3_c, final_ref, t_send, t1, t2, t3,
    load, wload, send1, recv1, csend, crecv, send2, recv2, c2send, c2recv, send3, recv3, tsend, trecv,
):
    stage = (st_a, st_b, st_c)
    q = (q_a, q_b, q_c)
    r1 = (r1_a, r1_b, r1_c)
    s2 = (s2_a, s2_b, s2_c)
    q2 = (q2_a, q2_b, q2_c)
    r2 = (r2_a, r2_b, r2_c)
    s3 = (s3_a, s3_b, s3_c)
    r3 = (r3_a, r3_b, r3_c)
    band = lax.axis_index("band")
    here = {
        "y": band // 8,
        "x": lax.rem(band // 2, 4),
        "c": lax.rem(band, 2),
        "z": lax.axis_index("sub"),
    }

    def peer(dim, shift, core=0):
        at = dict(here)
        at[dim] = lax.rem(here[dim] + shift, 4)
        at["c"] = lax.rem(here["c"] + core, 2)
        return at, ((at["y"] * 4 + at["x"]) * 2 + at["c"], at["z"])

    def remote(src, dst, send, recv, device):
        return pltpu.make_async_remote_copy(
            src_ref=src, dst_ref=dst, send_sem=send, recv_sem=recv,
            device_id=device, device_id_type=MESH,
        )

    loads = [
        pltpu.make_async_copy(slot_hbm, slot_ref, load.at[0]),
        pltpu.make_async_copy(target_hbm, target_ref, load.at[1]),
        pltpu.make_async_copy(mask_hbm, mask_ref, load.at[2]),
        pltpu.make_async_copy(fields_hbm, fields_ref, load.at[3]),
    ]
    size = BLOCKS // WEIGHT_COPIES
    weight_loads = [
        pltpu.make_async_copy(
            weights_hbm.at[pl.ds(i * size, size)], weights_ref.at[pl.ds(i * size, size)], wload.at[i]
        )
        for i in range(WEIGHT_COPIES)
    ]
    for copy in loads + weight_loads:
        copy.start()

    barrier = pltpu.get_barrier_semaphore()
    count = 0
    for dim in "zxy":
        for shift in (1, 2, 3):
            for core in (0, 1):
                pl.semaphore_signal(
                    barrier, inc=1, device_id=peer(dim, shift, core)[1], device_id_type=MESH
                )
                count += 1
    pl.semaphore_signal(barrier, inc=1, device_id=peer("z", 0, 1)[1], device_id_type=MESH)

    loads[0].wait()
    loads[1].wait()
    low = lax.broadcasted_iota(jnp.int32, (1, CELL), 1) < CHUNK
    blocks = lax.broadcasted_iota(jnp.int32, (8, BLOCKS), 1)
    kind = lax.broadcasted_iota(jnp.int32, (8, BLOCKS), 0)
    facts = jnp.where(kind == 0, blocks - BLOCKS, jnp.broadcast_to(target_ref[...], (8, BLOCKS)))
    facts = facts.astype(F32).astype(BF16)
    place = lax.broadcasted_iota(jnp.int32, (512, 1), 0)
    along = lax.broadcasted_iota(jnp.int32, (1, 512), 1)
    cs[...] = jnp.zeros_like(cs)
    for g in range(3):
        order = SLOTS[g]

        def split(n):
            chunk, second, third, k = n // 64, (n // 16) % 4, (n // 4) % 4, n % 4
            if g > 0:
                second = second + 1
            at = {
                order[0]: (here[order[0]] + chunk // 2) % 4,
                order[1]: (here[order[1]] + second) % 4,
                order[2]: (here[order[2]] + third) % 4,
                "c": (here["c"] + chunk) % 2,
            }
            return at, k

        at, k = split(place)
        wanted = (((at["y"] * 4 + at["x"]) * 2 + at["c"]) * 4 + at["z"]) * 4 + k
        hits = jnp.where(wanted == slot_ref[...], 1.0, 0.0).astype(BF16)
        found = lax.dot_general(
            facts, hits, (((1,), (1,)), ((), ())), preferred_element_type=F32
        )
        if g == 0:
            index_vmem[...] = (found[0:1] + BLOCKS).astype(jnp.int32)
            index_copy = pltpu.make_async_copy(index_vmem, index_smem, load.at[4])
            index_copy.start()
        at, k = split(along)
        owner = at[STAGES[g][1]] * 4 + at[STAGES[g][2]]
        code = found[1:2] + (owner * TARGETS).astype(F32)
        for pair in range(4):
            both = code[:, pair * CELL : (pair + 1) * CELL]
            rolled = pltpu.roll(both, CHUNK, 1)
            cs[g, 2 * pair, 0:1, :] = jnp.where(low, both, rolled)
            cs[g, 2 * pair + 1, 0:1, :] = jnp.where(low, rolled, both)

    loads[2].wait()
    loads[3].wait()
    live = live_ref[0]

    def build(i, total):
        for j in range(8):
            block = i * 8 + j
            alive = (block < live).astype(jnp.int32)
            mask = (mask_ref[pl.ds(block, 1), :] * alive).astype(F32)
            values = fields_ref[:, pl.ds(pl.multiple_of(block * CELL, CELL), CELL)].astype(F32)
            stacked = jnp.concatenate([values * mask, jnp.broadcast_to(mask, (4, CELL))], axis=0)
            total += stacked
            stack_ref[block] = stacked.astype(BF16)
        return total

    total = lax.fori_loop(0, BLOCKS // 8, build, jnp.zeros((16, CELL), F32))
    stack_ref[BLOCKS] = jnp.zeros((16, CELL), BF16)
    t_send[0] = total
    pl.semaphore_wait(barrier, count + 1)

    sends = []
    totals_first = []
    for slot in range(1, 8):
        copy = remote(
            t_send.at[0], t1.at[slot], tsend.at[0, slot], trecv.at[0, slot],
            peer("z", slot // 2, slot % 2)[1],
        )
        copy.start()
        sends.append(copy)
        totals_first.append(copy)
    index_copy.wait()
    for copy in weight_loads:
        copy.wait()

    def piece(g, slot, part, shift, core):
        return remote(
            q[g].at[slot, part], r1[g].at[slot, part], send1.at[g, slot], recv1.at[g, slot],
            peer(STAGES[g][0], shift, core)[1],
        )

    def step(s, carry):
        t = s // 2
        shift = lax.rem(t + 1, 4)
        core = 1 - lax.rem(s, 2)
        mine = shift * 2 + core

        def products(i, inner):
            for half in range(2):
                results = []
                for j in range(8):
                    block = jnp.clip(index_smem[0, mine * CHUNK + i * 16 + half * 8 + j], 0, BLOCKS)
                    results.append(
                        jnp.dot(
                            stack_ref[block],
                            weights_ref[jnp.minimum(block, BLOCKS - 1)],
                            preferred_element_type=F32,
                        )
                    )
                for j in range(8):
                    n = half * 8 + j
                    value = results[j]
                    st_a[pl.ds(i * 16 + n, 4, stride=64), :] = value[0:4]
                    st_b[pl.ds(i * 64 + n, 4, stride=16), :] = value[4:8]
                    st_c[pl.ds((n // 4) * 80 + i * 4 + n % 4, 5, stride=16), :] = value[8:13]
            return inner

        lax.fori_loop(0, 4, products, 0)
        whole = jnp.zeros((1, CELL), F32)
        for u in range(4):
            whole += encode(
                [st_a[r * 64 + u * 16 : r * 64 + u * 16 + 16, :] for r in range(4)],
                u * 16,
                lambda r, v: q_a.__setitem__((mine, u, r), v),
            )
        cs[0, mine, 1:2, :] = whole

        @pl.when(s < 7)
        def _():
            remote(
                q_a.at[mine], r1_a.at[mine], send1.at[0, mine], recv1.at[0, mine],
                peer("z", shift, core)[1],
            ).start()

        for g in (1, 2):
            rows = ROWS[g]
            for u in range(4):
                base = u * rows * 16
                slot = u * 2 + core
                cs[g, slot, 1:2, :] += encode(
                    [stage[g][base + r * 16 : base + r * 16 + 16, :] for r in range(rows)],
                    t * 16,
                    lambda r, v: q[g].__setitem__((slot, t, r), v),
                )
                if u == 0:

                    @pl.when(core == 1)
                    def _():
                        piece(g, slot, t, u, core).start()

                else:
                    piece(g, slot, t, u, core).start()
        return carry

    lax.fori_loop(0, 8, step, 0)

    first = [[None] * 8 for _ in range(3)]
    first_codes = [[None] * 8 for _ in range(3)]
    for slot in range(1, 8):
        for g in range(3):
            device = peer(STAGES[g][0], slot // 2, slot % 2)[1]
            copy = remote(
                cs.at[g, slot], c1.at[g, slot], csend.at[g, slot], crecv.at[g, slot], device
            )
            copy.start()
            first_codes[g][slot] = copy
            first[g][slot] = remote(
                q[g].at[slot], r1[g].at[slot], send1.at[g, slot], recv1.at[g, slot], device
            )
            sends += [copy, first[g][slot]]

    total = t_send[0]
    for slot, copy in enumerate(totals_first):
        copy.wait_recv()
        total += t1[slot + 1]
    t_send[1] = total
    totals_second = []
    for shift in (1, 2, 3):
        copy = remote(
            t_send.at[1], t2.at[shift - 1], tsend.at[1, shift], trecv.at[1, shift],
            peer("x", shift)[1],
        )
        copy.start()
        sends.append(copy)
        totals_second.append(copy)

    def join(rows):
        return jnp.concatenate(
            [jnp.where(low, rows[2 * p], rows[2 * p + 1]) for p in range(len(rows) // 2)], axis=1
        )

    second = []
    for g in range(3):
        for slot in range(1, 8):
            first_codes[g][slot].wait_recv()
            first[g][slot].wait_recv()
        heads = [cs[g, 0]] + [c1[g, slot] for slot in range(1, 8)]
        codes = join([h[0:1] for h in heads])
        scales = join([h[1:2] for h in heads])
        rows = lax.broadcasted_iota(jnp.int32, (256, 512), 0).astype(F32)
        select = jnp.where(rows == codes, scales, 0.0).astype(BF16)
        for row in range(ROWS[g]):
            data = jnp.concatenate(
                [
                    (q[g] if slot == 0 else r1[g])[slot, part, row]
                    for slot in range(8)
                    for part in range(4)
                ],
                axis=0,
            )
            both = jnp.dot(select, decode(data), preferred_element_type=F32)
            s2[g][row] = both[:, :CELL] + both[:, CELL:]
        for part in range(4):
            whole = jnp.zeros((1, CELL), F32)
            for u in range(4):
                base = part * 64 + u * 16
                whole += encode(
                    [s2[g][r, base : base + 16, :] for r in range(ROWS[g])],
                    u * 16,
                    lambda r, v: q2[g].__setitem__((part, u, r), v),
                )
            cs2[g, part, 0:1, :] = whole
        dim = STAGES[g][1]
        copies = []
        for shift in (2, 1, 3):
            at, device = peer(dim, shift)
            for src, dst, a, b in (
                (cs2.at[g, at[dim]], c2.at[g, shift], c2send, c2recv),
                (q2[g].at[at[dim]], r2[g].at[shift], send2, recv2),
            ):
                copy = remote(src, dst, a.at[g, shift], b.at[g, shift], device)
                copy.start()
                copies.append(copy)
        sends += copies
        second.append(copies)

    total = t_send[1]
    for shift in (1, 2, 3):
        totals_second[shift - 1].wait_recv()
        total += t2[shift - 1]
    t_send[2] = total
    totals_third = []
    for shift in (1, 2, 3):
        copy = remote(
            t_send.at[2], t3.at[shift - 1], tsend.at[2, shift], trecv.at[2, shift],
            peer("y", shift)[1],
        )
        copy.start()
        sends.append(copy)
        totals_third.append(copy)

    third = []
    for g in range(3):
        for copy in second[g]:
            copy.wait_recv()
        mine = here[STAGES[g][1]]
        scales = join([cs2[g, mine, 0:1, :]] + [c2[g, shift, 0:1, :] for shift in (1, 2, 3)])
        rows = lax.broadcasted_iota(jnp.int32, (64, 256), 0)
        lanes = lax.broadcasted_iota(jnp.int32, (64, 256), 1) % CHUNK
        select = jnp.where(rows == lanes, scales, 0.0).astype(BF16)
        for row in range(ROWS[g]):
            data = jnp.concatenate(
                [q2[g][mine, part, row] for part in range(4)]
                + [r2[g][shift, part, row] for shift in (1, 2, 3) for part in range(4)],
                axis=0,
            )
            both = jnp.dot(select, decode(data), preferred_element_type=F32)
            summed = both[:, :CELL] + both[:, CELL:]
            for part in range(4):
                s3[g][part, row] = summed[part * TARGETS : (part + 1) * TARGETS]
        dim = STAGES[g][2]
        copies = []
        for shift in (2, 1, 3):
            at, device = peer(dim, shift)
            copy = remote(
                s3[g].at[at[dim]], r3[g].at[shift - 1], send3.at[g, shift], recv3.at[g, shift], device
            )
            copy.start()
            copies.append(copy)
        sends += copies
        third.append(copies)

    total = t_send[2]
    for shift in (1, 2, 3):
        totals_third[shift - 1].wait_recv()
        total += t3[shift - 1]
    total = jnp.sum(total, axis=1, keepdims=True)
    mean = total[0:12] / jnp.maximum(total[12:13], 1.0)
    for g in range(3):
        for copy in third[g]:
            copy.wait_recv()
        mine = here[STAGES[g][2]]
        for row in range(ROWS[g]):
            summed = s3[g][mine, row] + r3[g][0, row] + r3[g][1, row] + r3[g][2, row]
            final_ref[pl.ds((FIRST[g] + row) * TARGETS, TARGETS), :] = summed
    for t in range(TARGETS):
        numer = final_ref[pl.ds(t, 12, stride=TARGETS), :]
        fraction = final_ref[pl.ds(12 * TARGETS + t, 1), :]
        filled = numer + jnp.maximum(0.25 - fraction, 0.0) * mean
        out_ref[:, t * CELL : (t + 1) * CELL] = filled / jnp.maximum(fraction, 0.25)
    for copy in sends:
        copy.wait_send()


def body(fields, land_mask, intersection, send_slot, target_block, live_blocks):
    smem = pl.BlockSpec(memory_space=pltpu.SMEM)
    hbm = pl.BlockSpec(memory_space=pl.ANY)
    dma = pltpu.SemaphoreType.DMA
    vmem = pltpu.VMEM
    i16 = jnp.int16
    i32 = jnp.int32
    return pl.pallas_call(
        kernel,
        in_specs=[smem] + [hbm] * 5,
        out_specs=pl.BlockSpec(memory_space=pltpu.VMEM),
        out_shape=jax.ShapeDtypeStruct((12, TARGETS * CELL), F32),
        scratch_shapes=[vmem((1, BLOCKS), i32), vmem((1, BLOCKS), i32)]
        + [vmem((12, BLOCKS * CELL), BF16), vmem((BLOCKS, CELL), i32)]
        + [vmem((BLOCKS, CELL, CELL), BF16), vmem((BLOCKS + 1, 16, CELL), BF16)]
        + [vmem((1, 512), i32), pltpu.SMEM((1, 512), i32)]
        + [vmem((n, CELL), F32) for n in (576, 336, 384)]
        + [vmem((8, 4, r, 16, CELL), i16) for r in ROWS] * 2
        + [vmem((3, 8, 8, CELL), F32)] * 2
        + [vmem((r, 256, CELL), F32) for r in ROWS]
        + [vmem((4, 4, r, 16, CELL), i16) for r in ROWS] * 2
        + [vmem((3, 4, 8, CELL), F32)] * 2
        + [vmem((4, r, TARGETS, CELL), F32) for r in ROWS]
        + [vmem((3, r, TARGETS, CELL), F32) for r in ROWS]
        + [vmem((13 * TARGETS, CELL), F32)]
        + [vmem((3, 16, CELL), F32), vmem((8, 16, CELL), F32)]
        + [vmem((3, 16, CELL), F32), vmem((3, 16, CELL), F32)]
        + [dma((5,)), dma((WEIGHT_COPIES,))]
        + [dma((3, 8))] * 4
        + [dma((3, 4))] * 6
        + [dma((3, 8))] * 2,
        compiler_params=pltpu.CompilerParams(
            collective_id=0, has_side_effects=True, vmem_limit_bytes=40 * 1024 * 1024
        ),
        name="remap",
    )(
        live_blocks,
        send_slot.reshape(1, BLOCKS),
        target_block.reshape(1, BLOCKS),
        fields,
        land_mask.reshape(BLOCKS, CELL),
        intersection,
    )


def solution(mesh):
    axes = ("band", "sub")
    return jax.shard_map(
        body,
        mesh=mesh,
        in_specs=(P(None, axes), P(axes), P(axes, None, None), P(axes), P(axes), P(axes)),
        out_specs=P(None, axes),
        check_vma=False,
    )
```

```python
import jax
import jax.numpy as jnp
from jax import lax
from jax.experimental import pallas as pl
from jax.experimental.pallas import tpu as pltpu
from jax.sharding import PartitionSpec as P

CELL = 128
BLOCKS = 256
TARGETS = 16
CHUNK = 64
ROWS = (4, 4, 5)
FIRST = (0, 4, 8)
STAGES = ("zxy", "xyz", "yzx")
SLOTS = ("zxy", "xzy", "yzx")
MESH = pl.DeviceIdType.MESH
F32 = jnp.float32
BF16 = jnp.bfloat16
WEIGHT_COPIES = 4


def encode(tiles, write):
    top = jnp.abs(tiles[0])
    for tile in tiles[1:]:
        top = jnp.maximum(top, jnp.abs(tile))
    top = jnp.maximum(jnp.max(top, axis=1, keepdims=True), 1e-25)
    power = jnp.ceil(jnp.log2(top) + 0.02)
    down = jnp.exp2(-power)
    for row, tile in enumerate(tiles):
        small = tile * down
        code = small * lax.rsqrt(jnp.abs(small) + 1e-30) * 32768.0
        write(row, jnp.round(code).astype(jnp.int32).astype(jnp.int16))
    return jnp.exp2(power - 30.0)


def spread(scale, period, lane):
    lanes = lax.broadcasted_iota(jnp.int32, (16, CELL), 1) % period
    slots = lax.broadcasted_iota(jnp.int32, (16, CELL), 0) + lane
    return jnp.sum(jnp.where(lanes == slots, scale, 0.0), axis=0, keepdims=True)


def decode(codes):
    value = codes.astype(F32)
    value = value * jnp.abs(value)
    high = value.astype(BF16)
    return jnp.concatenate([high, (value - high.astype(F32)).astype(BF16)], axis=1)


def kernel(
    live_ref, slot_hbm, target_hbm, fields_hbm, mask_hbm, weights_hbm, out_ref,
    slot_ref, target_ref, fields_ref, mask_ref, weights_ref, stack_ref, index_vmem, index_smem,
    even_a, even_b, even_c, odd_a, odd_b, odd_c, q_a, q_b, q_c, r1_a, r1_b, r1_c, cs, c1,
    s2_a, s2_b, s2_c, q2_a, q2_b, q2_c, r2_a, r2_b, r2_c, cs2, c2, final_ref, t_send, t1, t2,
    load, wload, send1, recv1, csend, crecv, send2, recv2, c2send, c2recv, tsend, trecv,
):
    stages = ((even_a, even_b, even_c), (odd_a, odd_b, odd_c))
    q = (q_a, q_b, q_c)
    r1 = (r1_a, r1_b, r1_c)
    s2 = (s2_a, s2_b, s2_c)
    q2 = (q2_a, q2_b, q2_c)
    r2 = (r2_a, r2_b, r2_c)
    band = lax.axis_index("band")
    here = {
        "y": band // 8,
        "x": lax.rem(band // 2, 4),
        "c": lax.rem(band, 2),
        "z": lax.axis_index("sub"),
    }

    def peer(**shifts):
        at = {}
        for dim in "yxcz":
            at[dim] = here[dim]
            if dim in shifts:
                at[dim] = lax.rem(here[dim] + shifts[dim], 2 if dim == "c" else 4)
        return at, ((at["y"] * 4 + at["x"]) * 2 + at["c"], at["z"])

    def remote(src, dst, send, recv, device):
        return pltpu.make_async_remote_copy(
            src_ref=src, dst_ref=dst, send_sem=send, recv_sem=recv,
            device_id=device, device_id_type=MESH,
        )

    partner = peer(c=1)[1]

    loads = [
        pltpu.make_async_copy(slot_hbm, slot_ref, load.at[0]),
        pltpu.make_async_copy(target_hbm, target_ref, load.at[1]),
        pltpu.make_async_copy(mask_hbm, mask_ref, load.at[2]),
        pltpu.make_async_copy(fields_hbm, fields_ref, load.at[3]),
    ]
    size = BLOCKS // WEIGHT_COPIES
    weight_loads = [
        pltpu.make_async_copy(
            weights_hbm.at[pl.ds(i * size, size)], weights_ref.at[pl.ds(i * size, size)], wload.at[i]
        )
        for i in range(WEIGHT_COPIES)
    ]
    for copy in loads + weight_loads:
        copy.start()

    barrier = pltpu.get_barrier_semaphore()
    greeted = set()
    for g in range(3):
        first, second, third = STAGES[g]
        for n in range(1, 8):
            greeted.add(tuple(sorted({first: n // 2, "c": n % 2}.items())))
        for n in range(1, 16):
            greeted.add(tuple(sorted({second: n // 4, third: n % 4}.items())))
    greeted = {tuple(item for item in names if item[1]) for names in greeted}
    for names in sorted(greeted):
        pl.semaphore_signal(
            barrier, inc=1, device_id=peer(**dict(names))[1], device_id_type=MESH
        )

    low = lax.broadcasted_iota(jnp.int32, (1, CELL), 1) < CHUNK
    blocks = lax.broadcasted_iota(jnp.int32, (8, BLOCKS), 1)
    kind = lax.broadcasted_iota(jnp.int32, (8, BLOCKS), 0)
    place = lax.broadcasted_iota(jnp.int32, (512, 1), 0)
    along = lax.broadcasted_iota(jnp.int32, (1, 512), 1)
    cs[...] = jnp.zeros_like(cs)
    loads[0].wait()
    loads[1].wait()
    facts = jnp.where(kind == 0, blocks - BLOCKS, jnp.broadcast_to(target_ref[...], (8, BLOCKS)))
    facts = facts.astype(F32).astype(BF16)
    for g in range(3):
        order = SLOTS[g]

        def split(n):
            chunk, second, third, k = n // 64, (n // 16) % 4, (n // 4) % 4, n % 4
            if g > 0:
                second = second + 1
            at = {
                order[0]: (here[order[0]] + chunk // 2) % 4,
                order[1]: (here[order[1]] + second) % 4,
                order[2]: (here[order[2]] + third) % 4,
                "c": (here["c"] + chunk) % 2,
            }
            return at, k

        at, k = split(place)
        wanted = (((at["y"] * 4 + at["x"]) * 2 + at["c"]) * 4 + at["z"]) * 4 + k
        hits = jnp.where(wanted == slot_ref[...], 1.0, 0.0).astype(BF16)
        found = lax.dot_general(
            facts, hits, (((1,), (1,)), ((), ())), preferred_element_type=F32
        )
        if g == 0:
            index_vmem[...] = (found[0:1] + BLOCKS).astype(jnp.int32)
            index_copy = pltpu.make_async_copy(index_vmem, index_smem, load.at[4])
            index_copy.start()
        at, k = split(along)
        owner = at[STAGES[g][1]] * 4 + at[STAGES[g][2]]
        code = found[1:2] + (owner * TARGETS).astype(F32)
        for pair in range(4):
            both = code[:, pair * CELL : (pair + 1) * CELL]
            rolled = pltpu.roll(both, CHUNK, 1)
            cs[g, 2 * pair, 0:1, :] = jnp.where(low, both, rolled)
            cs[g, 2 * pair + 1, 0:1, :] = jnp.where(low, rolled, both)

    loads[2].wait()
    loads[3].wait()
    live = live_ref[0]

    def build(i, total):
        for j in range(8):
            block = i * 8 + j
            alive = (block < live).astype(jnp.int32)
            mask = (mask_ref[pl.ds(block, 1), :] * alive).astype(F32)
            values = fields_ref[:, pl.ds(pl.multiple_of(block * CELL, CELL), CELL)].astype(F32)
            stacked = jnp.concatenate([values * mask, jnp.broadcast_to(mask, (4, CELL))], axis=0)
            total += stacked
            stack_ref[block] = stacked.astype(BF16)
        return total

    total = lax.fori_loop(0, BLOCKS // 8, build, jnp.zeros((16, CELL), F32))
    stack_ref[BLOCKS] = jnp.zeros((16, CELL), BF16)
    t_send[0] = total
    pl.semaphore_wait(barrier, len(greeted))

    for slot in range(1, 8):
        remote(
            t_send.at[0], t1.at[slot], tsend.at[0], trecv.at[0], peer(z=slot // 2, c=slot % 2)[1]
        ).start()
    index_copy.wait()
    for copy in weight_loads:
        copy.wait()

    def products(t, core, group):
        mine = lax.rem(t + 1, 4) * 2 + core
        stage = stages[core]
        results = []
        for j in range(8):
            at = mine * CHUNK + group * 8 + j
            block = jnp.clip(index_smem[0, at], 0, BLOCKS)
            results.append(
                jnp.dot(
                    stack_ref[block],
                    weights_ref[jnp.minimum(block, BLOCKS - 1)],
                    preferred_element_type=F32,
                )
            )
        for j in range(8):
            i, n = group // 2, (group % 2) * 8 + j
            value = results[j]
            stage[0][pl.ds(i * 16 + n, 4, stride=64), :] = value[0:4]
            stage[1][pl.ds(i * 64 + n, 4, stride=16), :] = value[4:8]
            stage[2][pl.ds((n // 4) * 80 + i * 4 + n % 4, 5, stride=16), :] = value[8:13]

    def code_tile(t, core, g, u, rows):
        stage = stages[core][g]
        if g == 0:
            mine = lax.rem(t + 1, 4) * 2 + core
            scale = encode(
                [stage[r * 64 + u * 16 : r * 64 + u * 16 + 16, :] for r in range(4)],
                lambda r, v: q_a.__setitem__((mine, u, r), v),
            )
            rows.append(spread(scale, CHUNK, u * 16))
        else:
            base = u * ROWS[g] * 16
            slot = u * 2 + core
            scale = encode(
                [stage[base + r * 16 : base + r * 16 + 16, :] for r in range(ROWS[g])],
                lambda r, v: q[g].__setitem__((slot, t, r), v),
            )
            cs[g, slot, 1:2, :] += spread(scale, CHUNK, t * 16)

    def ship(t, core, rows, home):
        shift = lax.rem(t + 1, 4)
        mine = shift * 2 + core
        cs[0, mine, 1:2, :] = (rows[0] + rows[1]) + (rows[2] + rows[3])
        if not home:
            remote(
                q_a.at[mine], r1_a.at[mine], send1.at[0], recv1.at[0], peer(z=shift, c=core)[1]
            ).start()
        for u in (2, 1, 3, 0):
            for g in (1, 2):
                if u or core:
                    slot = u * 2 + core
                    remote(
                        q[g].at[slot, t], r1[g].at[slot, t], send1.at[g], recv1.at[g],
                        peer(**{STAGES[g][0]: u, "c": core})[1],
                    ).start()

    tiles = [(g, u) for g in range(3) for u in range(4)]

    def together(ahead, behind, home=False):
        rows = []
        done = 0
        for group in range(8):
            if ahead is not None:
                products(*ahead, group)
            if behind is not None:
                upto = (group + 1) * len(tiles) // 8
                for g, u in tiles[done:upto]:
                    code_tile(*behind, g, u, rows)
                done = upto
        if behind is not None:
            ship(*behind, rows, home)

    together((0, 1), None)

    def step(t, carry):
        together((t, 0), (t, 1))
        together((t + 1, 1), (t, 0))
        return carry

    lax.fori_loop(0, 3, step, 0)
    together((3, 0), (3, 1))
    together(None, (3, 0), home=True)

    for slot in range(1, 8):
        for g in range(3):
            remote(
                cs.at[g, slot], c1.at[g, slot], csend.at[g], crecv.at[g],
                peer(**{STAGES[g][0]: slot // 2, "c": slot % 2})[1],
            ).start()

    def batch(src, dst, send, recv):
        return remote(src, dst, send, recv, partner)

    rest = pl.ds(1, 7)
    sums_first = batch(t1.at[rest], t1.at[rest], tsend.at[0], trecv.at[0])
    sums_first.wait_recv()
    total = t_send[0]
    for slot in range(1, 8):
        total += t1[slot]
    t_send[1] = total
    far = sorted(range(1, 16), key=lambda n: -(min(n // 4, 4 - n // 4) + min(n % 4, 4 - n % 4)))
    for n in far:
        remote(
            t_send.at[1], t2.at[n], tsend.at[1], trecv.at[1], peer(x=n // 4, y=n % 4)[1]
        ).start()

    ends = [sums_first]
    others = pl.ds(1, 15)
    for g in range(3):
        heads = batch(cs.at[g, rest], c1.at[g, rest], csend.at[g], crecv.at[g])
        datas = batch(q[g].at[rest], r1[g].at[rest], send1.at[g], recv1.at[g])
        heads.wait_recv()
        datas.wait_recv()
        ends += [heads, datas]
        head = [cs[g, 0]] + [c1[g, slot] for slot in range(1, 8)]

        def lane_row(at):
            return jnp.concatenate(
                [
                    jnp.where(low, head[2 * p][at : at + 1], head[2 * p + 1][at : at + 1])
                    for p in range(4)
                ],
                axis=1,
            )

        rows = lax.broadcasted_iota(jnp.int32, (256, 512), 0).astype(F32)
        select = jnp.where(rows == lane_row(0), lane_row(1), 0.0).astype(BF16)
        for row in range(ROWS[g]):
            data = jnp.concatenate(
                [
                    (q[g] if slot == 0 else r1[g])[slot, part, row]
                    for slot in range(8)
                    for part in range(4)
                ],
                axis=0,
            )
            both = jnp.dot(select, decode(data), preferred_element_type=F32)
            s2[g][row] = both[:, :CELL] + both[:, CELL:]
        for owner in range(16):
            scale = encode(
                [s2[g][r, owner * 16 : owner * 16 + 16, :] for r in range(ROWS[g])],
                lambda r, v: q2[g].__setitem__((owner, r), v),
            )
            cs2[g, owner, 0:1, :] = spread(scale, 16, 0)
        second, third = STAGES[g][1:]
        for n in far:
            at, device = peer(**{second: n // 4, third: n % 4})
            owner = at[second] * 4 + at[third]
            remote(
                cs2.at[g, owner], c2.at[g, n], c2send.at[g], c2recv.at[g], device
            ).start()
            remote(q2[g].at[owner], r2[g].at[n], send2.at[g], recv2.at[g], device).start()

    sums_second = batch(t2.at[others], t2.at[others], tsend.at[1], trecv.at[1])
    sums_second.wait_recv()
    ends.append(sums_second)
    total = t_send[1]
    for n in range(1, 16):
        total += t2[n]
    total = jnp.sum(total, axis=1, keepdims=True)
    mean = total[0:12] / jnp.maximum(total[12:13], 1.0)
    group_of = lax.broadcasted_iota(jnp.int32, (1, CELL), 1) // 16
    for g in range(3):
        heads = batch(c2.at[g, others], c2.at[g, others], c2send.at[g], c2recv.at[g])
        datas = batch(r2[g].at[others], r2[g].at[others], send2.at[g], recv2.at[g])
        heads.wait_recv()
        datas.wait_recv()
        ends += [heads, datas]
        mine = here[STAGES[g][1]] * 4 + here[STAGES[g][2]]
        halves = []
        for half in range(2):
            row = jnp.zeros((1, CELL), F32)
            for n in range(8):
                source = cs2[g, mine, 0:1, :] if half + n == 0 else c2[g, half * 8 + n, 0:1, :]
                row = jnp.where(group_of == n, source, row)
            halves.append(row)
        scales = jnp.concatenate(halves, axis=1)
        rows = lax.broadcasted_iota(jnp.int32, (16, 256), 0)
        lanes = lax.broadcasted_iota(jnp.int32, (16, 256), 1) % 16
        select = jnp.where(rows == lanes, scales, 0.0).astype(BF16)
        for row in range(ROWS[g]):
            data = jnp.concatenate(
                [q2[g][mine, row]] + [r2[g][n, row] for n in range(1, 16)], axis=0
            )
            both = jnp.dot(select, decode(data), preferred_element_type=F32)
            final_ref[pl.ds((FIRST[g] + row) * TARGETS, TARGETS), :] = (
                both[:, :CELL] + both[:, CELL:]
            )
    for t in range(TARGETS):
        numer = final_ref[pl.ds(t, 12, stride=TARGETS), :]
        fraction = final_ref[pl.ds(12 * TARGETS + t, 1), :]
        filled = numer + jnp.maximum(0.25 - fraction, 0.0) * mean
        out_ref[:, t * CELL : (t + 1) * CELL] = filled / jnp.maximum(fraction, 0.25)
    for copy in ends:
        copy.wait_send()


def body(fields, land_mask, intersection, send_slot, target_block, live_blocks):
    smem = pl.BlockSpec(memory_space=pltpu.SMEM)
    hbm = pl.BlockSpec(memory_space=pl.ANY)
    dma = pltpu.SemaphoreType.DMA
    vmem = pltpu.VMEM
    i16 = jnp.int16
    i32 = jnp.int32
    return pl.pallas_call(
        kernel,
        in_specs=[smem] + [hbm] * 5,
        out_specs=pl.BlockSpec(memory_space=pltpu.VMEM),
        out_shape=jax.ShapeDtypeStruct((12, TARGETS * CELL), F32),
        scratch_shapes=[vmem((1, BLOCKS), i32), vmem((1, BLOCKS), i32)]
        + [vmem((12, BLOCKS * CELL), BF16), vmem((BLOCKS, CELL), i32)]
        + [vmem((BLOCKS, CELL, CELL), BF16), vmem((BLOCKS + 1, 16, CELL), BF16)]
        + [vmem((1, 512), i32), pltpu.SMEM((1, 512), i32)]
        + [vmem((n, CELL), F32) for n in (576, 336, 384)] * 2
        + [vmem((8, 4, r, 16, CELL), i16) for r in ROWS] * 2
        + [vmem((3, 8, 8, CELL), F32)] * 2
        + [vmem((r, 256, CELL), F32) for r in ROWS]
        + [vmem((16, r, 16, CELL), i16) for r in ROWS] * 2
        + [vmem((3, 16, 8, CELL), F32)] * 2
        + [vmem((16 * TARGETS, CELL), F32)]
        + [vmem((2, 16, CELL), F32), vmem((8, 16, CELL), F32), vmem((16, 16, CELL), F32)]
        + [dma((5,)), dma((WEIGHT_COPIES,))]
        + [dma((3,))] * 8
        + [dma((2,))] * 2,
        compiler_params=pltpu.CompilerParams(
            collective_id=0, has_side_effects=True, vmem_limit_bytes=62 * 1024 * 1024
        ),
        name="remap",
    )(
        live_blocks,
        send_slot.reshape(1, BLOCKS),
        target_block.reshape(1, BLOCKS),
        fields,
        land_mask.reshape(BLOCKS, CELL),
        intersection,
    )


def solution(mesh):
    axes = ("band", "sub")
    return jax.shard_map(
        body,
        mesh=mesh,
        in_specs=(P(None, axes), P(axes), P(axes, None, None), P(axes), P(axes), P(axes)),
        out_specs=P(None, axes),
        check_vma=False,
    )
```

```python
import jax
import jax.numpy as jnp
from jax import lax
from jax.experimental import pallas as pl
from jax.experimental.pallas import tpu as pltpu
from jax.sharding import PartitionSpec as P

CELL = 128
BLOCKS = 256
TARGETS = 16
CHUNK = 64
ROWS = (4, 4, 5)
FIRST = (0, 4, 8)
STAGES = ("zxy", "xyz", "yzx")
SLOTS = ("zxy", "xzy", "yzx")
MESH = pl.DeviceIdType.MESH
F32 = jnp.float32
BF16 = jnp.bfloat16
WEIGHT_COPIES = 4


def encode(tiles, write):
    top = jnp.abs(tiles[0])
    for tile in tiles[1:]:
        top = jnp.maximum(top, jnp.abs(tile))
    top = jnp.maximum(jnp.max(top, axis=1, keepdims=True), 1e-25)
    power = jnp.ceil(jnp.log2(top) + 0.02)
    down = jnp.exp2(-power)
    for row, tile in enumerate(tiles):
        small = tile * down
        code = small * lax.rsqrt(jnp.abs(small) + 1e-30) * 32768.0
        write(row, jnp.round(code).astype(jnp.int32).astype(jnp.int16))
    return jnp.exp2(power - 30.0)


def spread(scale, period, lane):
    lanes = lax.broadcasted_iota(jnp.int32, (16, CELL), 1) % period
    slots = lax.broadcasted_iota(jnp.int32, (16, CELL), 0) + lane
    return jnp.sum(jnp.where(lanes == slots, scale, 0.0), axis=0, keepdims=True)


def decode(codes):
    value = codes.astype(F32)
    value = value * jnp.abs(value)
    high = value.astype(BF16)
    return jnp.concatenate([high, (value - high.astype(F32)).astype(BF16)], axis=1)


def kernel(
    live_ref, slot_hbm, target_hbm, fields_hbm, mask_hbm, weights_hbm, out_ref,
    slot_ref, target_ref, fields_ref, mask_ref, weights_ref, stack_ref, index_vmem, index_smem,
    even_a, even_b, even_c, odd_a, odd_b, odd_c, q_a, q_b, q_c, r1_a, r1_b, r1_c, cs, c1,
    s2_a, s2_b, s2_c, q2_a, q2_b, q2_c, r2_a, r2_b, r2_c, cs2, c2, final_ref, t_send, t1, t2,
    load, wload, send1, recv1, csend, crecv, send2, recv2, c2send, c2recv, tsend, trecv,
):
    stages = ((even_a, even_b, even_c), (odd_a, odd_b, odd_c))
    q = (q_a, q_b, q_c)
    r1 = (r1_a, r1_b, r1_c)
    s2 = (s2_a, s2_b, s2_c)
    q2 = (q2_a, q2_b, q2_c)
    r2 = (r2_a, r2_b, r2_c)
    band = lax.axis_index("band")
    here = {
        "y": band // 8,
        "x": lax.rem(band // 2, 4),
        "c": lax.rem(band, 2),
        "z": lax.axis_index("sub"),
    }

    def peer(**shifts):
        at = {}
        for dim in "yxcz":
            at[dim] = here[dim]
            if dim in shifts:
                at[dim] = lax.rem(here[dim] + shifts[dim], 2 if dim == "c" else 4)
        return at, ((at["y"] * 4 + at["x"]) * 2 + at["c"], at["z"])

    def remote(src, dst, send, recv, device):
        return pltpu.make_async_remote_copy(
            src_ref=src, dst_ref=dst, send_sem=send, recv_sem=recv,
            device_id=device, device_id_type=MESH,
        )

    partner = peer(c=1)[1]

    def reach(t):
        near = 1 + 2 * here["c"]
        return jnp.where(t == 0, 2, jnp.where(t == 1, near, jnp.where(t == 2, 4 - near, 0)))

    loads = [
        pltpu.make_async_copy(slot_hbm, slot_ref, load.at[0]),
        pltpu.make_async_copy(target_hbm, target_ref, load.at[1]),
        pltpu.make_async_copy(mask_hbm, mask_ref, load.at[2]),
        pltpu.make_async_copy(fields_hbm, fields_ref, load.at[3]),
    ]
    size = BLOCKS // WEIGHT_COPIES
    weight_loads = [
        pltpu.make_async_copy(
            weights_hbm.at[pl.ds(i * size, size)], weights_ref.at[pl.ds(i * size, size)], wload.at[i]
        )
        for i in range(WEIGHT_COPIES)
    ]
    for copy in loads + weight_loads:
        copy.start()

    barrier = pltpu.get_barrier_semaphore()
    greeted = set()
    for g in range(3):
        first, second, third = STAGES[g]
        for n in range(1, 8):
            greeted.add(tuple(sorted({first: n // 2, "c": n % 2}.items())))
        for n in range(1, 16):
            greeted.add(tuple(sorted({second: n // 4, third: n % 4}.items())))
    greeted = {tuple(item for item in names if item[1]) for names in greeted}
    for names in sorted(greeted):
        pl.semaphore_signal(
            barrier, inc=1, device_id=peer(**dict(names))[1], device_id_type=MESH
        )

    low = lax.broadcasted_iota(jnp.int32, (1, CELL), 1) < CHUNK
    blocks = lax.broadcasted_iota(jnp.int32, (8, BLOCKS), 1)
    kind = lax.broadcasted_iota(jnp.int32, (8, BLOCKS), 0)
    place = lax.broadcasted_iota(jnp.int32, (512, 1), 0)
    along = lax.broadcasted_iota(jnp.int32, (1, 512), 1)
    cs[...] = jnp.zeros_like(cs)
    loads[0].wait()
    loads[1].wait()
    facts = jnp.where(kind == 0, blocks - BLOCKS, jnp.broadcast_to(target_ref[...], (8, BLOCKS)))
    facts = facts.astype(F32).astype(BF16)
    index_copy = pltpu.make_async_copy(index_vmem, index_smem, load.at[4])

    def fill(g):
        order = SLOTS[g]

        def split(n):
            chunk, second, third, k = n // 64, (n // 16) % 4, (n // 4) % 4, n % 4
            if g > 0:
                second = reach(second)
            at = {
                order[0]: (here[order[0]] + chunk // 2) % 4,
                order[1]: (here[order[1]] + second) % 4,
                order[2]: (here[order[2]] + third) % 4,
                "c": (here["c"] + chunk) % 2,
            }
            return at, k

        at, k = split(place)
        wanted = (((at["y"] * 4 + at["x"]) * 2 + at["c"]) * 4 + at["z"]) * 4 + k
        hits = jnp.where(wanted == slot_ref[...], 1.0, 0.0).astype(BF16)
        found = lax.dot_general(
            facts, hits, (((1,), (1,)), ((), ())), preferred_element_type=F32
        )
        if g == 0:
            index_vmem[...] = (found[0:1] + BLOCKS).astype(jnp.int32)
            index_copy.start()
        at, k = split(along)
        owner = at[STAGES[g][1]] * 4 + at[STAGES[g][2]]
        code = found[1:2] + (owner * TARGETS).astype(F32)
        for pair in range(4):
            both = code[:, pair * CELL : (pair + 1) * CELL]
            rolled = pltpu.roll(both, CHUNK, 1)
            cs[g, 2 * pair, 0:1, :] = jnp.where(low, both, rolled)
            cs[g, 2 * pair + 1, 0:1, :] = jnp.where(low, rolled, both)

    fill(0)

    loads[2].wait()
    loads[3].wait()
    live = live_ref[0]

    def build(i, total):
        for j in range(8):
            block = i * 8 + j
            alive = (block < live).astype(jnp.int32)
            mask = (mask_ref[pl.ds(block, 1), :] * alive).astype(F32)
            values = fields_ref[:, pl.ds(pl.multiple_of(block * CELL, CELL), CELL)].astype(F32)
            stacked = jnp.concatenate([values * mask, jnp.broadcast_to(mask, (4, CELL))], axis=0)
            total += stacked
            stack_ref[block] = stacked.astype(BF16)
        return total

    total = lax.fori_loop(0, BLOCKS // 8, build, jnp.zeros((16, CELL), F32))
    stack_ref[BLOCKS] = jnp.zeros((16, CELL), BF16)
    t_send[0] = spread(jnp.sum(total, axis=1, keepdims=True), CELL, 0)
    pl.semaphore_wait(barrier, len(greeted))

    for slot in range(1, 8):
        remote(
            t_send.at[0], t1.at[slot], tsend.at[0], trecv.at[0], peer(z=slot // 2, c=slot % 2)[1]
        ).start()
    index_copy.wait()
    for copy in weight_loads:
        copy.wait()

    def products(t, core, group):
        mine = reach(t) * 2 + core
        stage = stages[core]
        results = []
        for j in range(8):
            at = mine * CHUNK + group * 8 + j
            block = jnp.clip(index_smem[0, at], 0, BLOCKS)
            results.append(
                jnp.dot(
                    stack_ref[block],
                    weights_ref[jnp.minimum(block, BLOCKS - 1)],
                    preferred_element_type=F32,
                )
            )
        for j in range(8):
            i, n = group // 2, (group % 2) * 8 + j
            value = results[j]
            stage[0][pl.ds(i * 16 + n, 4, stride=64), :] = value[0:4]
            stage[1][pl.ds(i * 64 + n, 4, stride=16), :] = value[4:8]
            stage[2][pl.ds((n // 4) * 80 + i * 4 + n % 4, 5, stride=16), :] = value[8:13]

    def code_tile(t, core, g, u, rows):
        stage = stages[core][g]
        if g == 0:
            mine = reach(t) * 2 + core
            scale = encode(
                [stage[r * 64 + u * 16 : r * 64 + u * 16 + 16, :] for r in range(4)],
                lambda r, v: q_a.__setitem__((mine, u, r), v),
            )
            rows.append(spread(scale, CHUNK, u * 16))
        else:
            base = u * ROWS[g] * 16
            slot = u * 2 + core
            scale = encode(
                [stage[base + r * 16 : base + r * 16 + 16, :] for r in range(ROWS[g])],
                lambda r, v: q[g].__setitem__((slot, t, r), v),
            )
            cs[g, slot, 1:2, :] += spread(scale, CHUNK, t * 16)

    def ship(t, core, rows, home):
        shift = reach(t)
        mine = shift * 2 + core
        cs[0, mine, 1:2, :] = (rows[0] + rows[1]) + (rows[2] + rows[3])
        if not home:
            remote(
                cs.at[0, mine], c1.at[0, mine], csend.at[0], crecv.at[0], peer(z=shift, c=core)[1]
            ).start()
            remote(
                q_a.at[mine], r1_a.at[mine], send1.at[0], recv1.at[0], peer(z=shift, c=core)[1]
            ).start()
        for u in (2, 1, 3, 0):
            for g in (1, 2):
                if u or core:
                    slot = u * 2 + core
                    remote(
                        q[g].at[slot, t], r1[g].at[slot, t], send1.at[g], recv1.at[g],
                        peer(**{STAGES[g][0]: u, "c": core})[1],
                    ).start()

    tiles = [(g, u) for g in range(3) for u in range(4)]

    def together(ahead, behind, home=False, extra=False):
        rows = []
        done = 0
        for group in range(8):
            if ahead is not None:
                products(*ahead, group)
            if extra and group in (2, 5):
                fill(1 + group // 5)
            if behind is not None:
                upto = (group + 1) * len(tiles) // 8
                for g, u in tiles[done:upto]:
                    code_tile(*behind, g, u, rows)
                done = upto
        if behind is not None:
            ship(*behind, rows, home)

    together((0, 1), None, extra=True)

    def step(t, carry):
        together((t, 0), (t, 1))
        together((t + 1, 1), (t, 0))
        return carry

    lax.fori_loop(0, 3, step, 0)
    together((3, 0), (3, 1))
    together(None, (3, 0), home=True)

    for slot in range(1, 8):
        for g in (1, 2):
            remote(
                cs.at[g, slot], c1.at[g, slot], csend.at[g], crecv.at[g],
                peer(**{STAGES[g][0]: slot // 2, "c": slot % 2})[1],
            ).start()

    def batch(src, dst, send, recv):
        return remote(src, dst, send, recv, partner)

    rest = pl.ds(1, 7)
    sums_first = batch(t1.at[rest], t1.at[rest], tsend.at[0], trecv.at[0])
    sums_first.wait_recv()
    total = t_send[0]
    for slot in range(1, 8):
        total += t1[slot]
    t_send[1] = total
    far = sorted(range(1, 16), key=lambda n: -(min(n // 4, 4 - n // 4) + min(n % 4, 4 - n % 4)))
    for n in far:
        remote(
            t_send.at[1], t2.at[n], tsend.at[1], trecv.at[1], peer(x=n // 4, y=n % 4)[1]
        ).start()

    ends = [sums_first]
    others = pl.ds(1, 15)
    for g in range(3):
        heads = batch(cs.at[g, rest], c1.at[g, rest], csend.at[g], crecv.at[g])
        datas = batch(q[g].at[rest], r1[g].at[rest], send1.at[g], recv1.at[g])
        heads.wait_recv()
        datas.wait_recv()
        ends += [heads, datas]
        head = [cs[g, 0]] + [c1[g, slot] for slot in range(1, 8)]

        def lane_row(at):
            return jnp.concatenate(
                [
                    jnp.where(low, head[2 * p][at : at + 1], head[2 * p + 1][at : at + 1])
                    for p in range(4)
                ],
                axis=1,
            )

        rows = lax.broadcasted_iota(jnp.int32, (256, 512), 0).astype(F32)
        select = jnp.where(rows == lane_row(0), lane_row(1), 0.0).astype(BF16)
        for row in range(ROWS[g]):
            data = jnp.concatenate(
                [
                    (q[g] if slot == 0 else r1[g])[slot, part, row]
                    for slot in range(8)
                    for part in range(4)
                ],
                axis=0,
            )
            both = jnp.dot(select, decode(data), preferred_element_type=F32)
            s2[g][row] = both[:, :CELL] + both[:, CELL:]
        for owner in range(16):
            scale = encode(
                [s2[g][r, owner * 16 : owner * 16 + 16, :] for r in range(ROWS[g])],
                lambda r, v: q2[g].__setitem__((owner, r), v),
            )
            cs2[g, owner, 0:1, :] = spread(scale, 16, 0)
        second, third = STAGES[g][1:]
        for n in far:
            at, device = peer(**{second: n // 4, third: n % 4})
            owner = at[second] * 4 + at[third]
            remote(
                cs2.at[g, owner], c2.at[g, n], c2send.at[g], c2recv.at[g], device
            ).start()
            remote(q2[g].at[owner], r2[g].at[n], send2.at[g], recv2.at[g], device).start()

    sums_second = batch(t2.at[others], t2.at[others], tsend.at[1], trecv.at[1])
    sums_second.wait_recv()
    ends.append(sums_second)
    total = t_send[1]
    for n in range(1, 16):
        total += t2[n]
    lanes = lax.broadcasted_iota(jnp.int32, (16, CELL), 1)
    rows = lax.broadcasted_iota(jnp.int32, (16, CELL), 0)
    total = jnp.sum(jnp.where(lanes == rows, total, 0.0), axis=1, keepdims=True)
    mean = total[0:12] / jnp.maximum(total[12:13], 1.0)
    group_of = lax.broadcasted_iota(jnp.int32, (1, CELL), 1) // 16
    for g in range(3):
        heads = batch(c2.at[g, others], c2.at[g, others], c2send.at[g], c2recv.at[g])
        datas = batch(r2[g].at[others], r2[g].at[others], send2.at[g], recv2.at[g])
        heads.wait_recv()
        datas.wait_recv()
        ends += [heads, datas]
        mine = here[STAGES[g][1]] * 4 + here[STAGES[g][2]]
        halves = []
        for half in range(2):
            row = jnp.zeros((1, CELL), F32)
            for n in range(8):
                source = cs2[g, mine, 0:1, :] if half + n == 0 else c2[g, half * 8 + n, 0:1, :]
                row = jnp.where(group_of == n, source, row)
            halves.append(row)
        scales = jnp.concatenate(halves, axis=1)
        rows = lax.broadcasted_iota(jnp.int32, (16, 256), 0)
        lanes = lax.broadcasted_iota(jnp.int32, (16, 256), 1) % 16
        select = jnp.where(rows == lanes, scales, 0.0).astype(BF16)
        for row in range(ROWS[g]):
            data = jnp.concatenate(
                [q2[g][mine, row]] + [r2[g][n, row] for n in range(1, 16)], axis=0
            )
            both = jnp.dot(select, decode(data), preferred_element_type=F32)
            final_ref[pl.ds((FIRST[g] + row) * TARGETS, TARGETS), :] = (
                both[:, :CELL] + both[:, CELL:]
            )
    for t in range(TARGETS):
        numer = final_ref[pl.ds(t, 12, stride=TARGETS), :]
        fraction = final_ref[pl.ds(12 * TARGETS + t, 1), :]
        filled = numer + jnp.maximum(0.25 - fraction, 0.0) * mean
        out_ref[:, t * CELL : (t + 1) * CELL] = filled / jnp.maximum(fraction, 0.25)
    for copy in ends:
        copy.wait_send()


def body(fields, land_mask, intersection, send_slot, target_block, live_blocks):
    smem = pl.BlockSpec(memory_space=pltpu.SMEM)
    hbm = pl.BlockSpec(memory_space=pl.ANY)
    dma = pltpu.SemaphoreType.DMA
    vmem = pltpu.VMEM
    i16 = jnp.int16
    i32 = jnp.int32
    return pl.pallas_call(
        kernel,
        in_specs=[smem] + [hbm] * 5,
        out_specs=pl.BlockSpec(memory_space=pltpu.VMEM),
        out_shape=jax.ShapeDtypeStruct((12, TARGETS * CELL), F32),
        scratch_shapes=[vmem((1, BLOCKS), i32), vmem((1, BLOCKS), i32)]
        + [vmem((12, BLOCKS * CELL), BF16), vmem((BLOCKS, CELL), i32)]
        + [vmem((BLOCKS, CELL, CELL), BF16), vmem((BLOCKS + 1, 16, CELL), BF16)]
        + [vmem((1, 512), i32), pltpu.SMEM((1, 512), i32)]
        + [vmem((n, CELL), F32) for n in (576, 336, 384)] * 2
        + [vmem((8, 4, r, 16, CELL), i16) for r in ROWS] * 2
        + [vmem((3, 8, 2, CELL), F32)] * 2
        + [vmem((r, 256, CELL), F32) for r in ROWS]
        + [vmem((16, r, 16, CELL), i16) for r in ROWS] * 2
        + [vmem((3, 16, 1, CELL), F32)] * 2
        + [vmem((16 * TARGETS, CELL), F32)]
        + [vmem((2, 1, CELL), F32), vmem((8, 1, CELL), F32), vmem((16, 1, CELL), F32)]
        + [dma((5,)), dma((WEIGHT_COPIES,))]
        + [dma((3,))] * 8
        + [dma((2,))] * 2,
        compiler_params=pltpu.CompilerParams(
            collective_id=0, has_side_effects=True, vmem_limit_bytes=62 * 1024 * 1024
        ),
        name="remap",
    )(
        live_blocks,
        send_slot.reshape(1, BLOCKS),
        target_block.reshape(1, BLOCKS),
        fields,
        land_mask.reshape(BLOCKS, CELL),
        intersection,
    )


def solution(mesh):
    axes = ("band", "sub")
    return jax.shard_map(
        body,
        mesh=mesh,
        in_specs=(P(None, axes), P(axes), P(axes, None, None), P(axes), P(axes), P(axes)),
        out_specs=P(None, axes),
        check_vma=False,
    )
```

```python
import jax
import jax.numpy as jnp
from jax import lax
from jax.experimental import pallas as pl
from jax.experimental.pallas import tpu as pltpu
from jax.sharding import PartitionSpec as P

CELL = 128
BLOCKS = 256
TARGETS = 16
CHUNK = 64
ROWS = (4, 4, 5)
FIRST = (0, 4, 8)
STAGES = ("zxy", "xyz", "yzx")
SLOTS = ("zxy", "xzy", "yzx")
MESH = pl.DeviceIdType.MESH
F32 = jnp.float32
BF16 = jnp.bfloat16
WEIGHT_COPIES = 1


def encode(tiles, write):
    top = jnp.abs(tiles[0])
    for tile in tiles[1:]:
        top = jnp.maximum(top, jnp.abs(tile))
    top = jnp.maximum(jnp.max(top, axis=1, keepdims=True), 1e-25)
    power = jnp.ceil(jnp.log2(top) + 0.02)
    down = jnp.exp2(-power)
    for row, tile in enumerate(tiles):
        small = tile * down
        code = small * lax.rsqrt(jnp.abs(small) + 1e-30) * 32768.0
        write(row, jnp.round(code).astype(jnp.int32).astype(jnp.int16))
    return jnp.exp2(power - 30.0)


def spread(scale, period, lane):
    lanes = lax.broadcasted_iota(jnp.int32, (16, CELL), 1) % period
    slots = lax.broadcasted_iota(jnp.int32, (16, CELL), 0) + lane
    return jnp.sum(jnp.where(lanes == slots, scale, 0.0), axis=0, keepdims=True)


def decode(codes):
    value = codes.astype(F32)
    value = value * jnp.abs(value)
    high = value.astype(BF16)
    return jnp.concatenate([high, (value - high.astype(F32)).astype(BF16)], axis=1)


def kernel(
    live_ref, slot_hbm, target_hbm, fields_hbm, mask_hbm, weights_hbm, out_ref,
    slot_ref, target_ref, fields_ref, mask_ref, weights_ref, stack_ref, index_vmem, index_smem,
    even_a, even_b, even_c, odd_a, odd_b, odd_c, q_a, q_b, q_c, r1_a, r1_b, r1_c, cs, c1,
    s2_a, s2_b, s2_c, q2_a, q2_b, q2_c, r2_a, r2_b, r2_c, cs2, c2, final_ref, t_send, t1, t2,
    load, wload, send1, recv1, csend, crecv, send2, recv2, c2send, c2recv, tsend, trecv,
):
    stages = ((even_a, even_b, even_c), (odd_a, odd_b, odd_c))
    q = (q_a, q_b, q_c)
    r1 = (r1_a, r1_b, r1_c)
    s2 = (s2_a, s2_b, s2_c)
    q2 = (q2_a, q2_b, q2_c)
    r2 = (r2_a, r2_b, r2_c)
    band = lax.axis_index("band")
    here = {
        "y": band // 8,
        "x": lax.rem(band // 2, 4),
        "c": lax.rem(band, 2),
        "z": lax.axis_index("sub"),
    }

    def peer(**shifts):
        at = {}
        for dim in "yxcz":
            at[dim] = here[dim]
            if dim in shifts:
                at[dim] = lax.rem(here[dim] + shifts[dim], 2 if dim == "c" else 4)
        return at, ((at["y"] * 4 + at["x"]) * 2 + at["c"], at["z"])

    def remote(src, dst, send, recv, device):
        return pltpu.make_async_remote_copy(
            src_ref=src, dst_ref=dst, send_sem=send, recv_sem=recv,
            device_id=device, device_id_type=MESH,
        )

    partner = peer(c=1)[1]

    def reach(t):
        near = 1 + 2 * here["c"]
        return jnp.where(t == 0, 2, jnp.where(t == 1, near, jnp.where(t == 2, 4 - near, 0)))

    loads = [
        pltpu.make_async_copy(slot_hbm, slot_ref, load.at[0]),
        pltpu.make_async_copy(target_hbm, target_ref, load.at[1]),
        pltpu.make_async_copy(mask_hbm, mask_ref, load.at[2]),
        pltpu.make_async_copy(fields_hbm, fields_ref, load.at[3]),
    ]
    size = BLOCKS // WEIGHT_COPIES
    weight_loads = [
        pltpu.make_async_copy(
            weights_hbm.at[pl.ds(i * size, size)], weights_ref.at[pl.ds(i * size, size)], wload.at[i]
        )
        for i in range(WEIGHT_COPIES)
    ]
    for copy in loads + weight_loads:
        copy.start()

    barrier = pltpu.get_barrier_semaphore()
    greeted = set()
    for g in range(3):
        first, second, third = STAGES[g]
        for n in range(1, 8):
            greeted.add(tuple(sorted({first: n // 2, "c": n % 2}.items())))
        for n in range(1, 16):
            greeted.add(tuple(sorted({second: n // 4, third: n % 4}.items())))
    greeted = {tuple(item for item in names if item[1]) for names in greeted}
    for names in sorted(greeted):
        pl.semaphore_signal(
            barrier, inc=1, device_id=peer(**dict(names))[1], device_id_type=MESH
        )

    low = lax.broadcasted_iota(jnp.int32, (1, CELL), 1) < CHUNK
    blocks = lax.broadcasted_iota(jnp.int32, (8, BLOCKS), 1)
    kind = lax.broadcasted_iota(jnp.int32, (8, BLOCKS), 0)
    place = lax.broadcasted_iota(jnp.int32, (512, 1), 0)
    along = lax.broadcasted_iota(jnp.int32, (1, 512), 1)
    cs[...] = jnp.zeros_like(cs)
    loads[0].wait()
    loads[1].wait()
    facts = jnp.where(kind == 0, blocks - BLOCKS, jnp.broadcast_to(target_ref[...], (8, BLOCKS)))
    facts = facts.astype(F32).astype(BF16)
    index_copy = pltpu.make_async_copy(index_vmem, index_smem, load.at[4])

    def fill(g):
        order = SLOTS[g]

        def split(n):
            chunk, second, third, k = n // 64, (n // 16) % 4, (n // 4) % 4, n % 4
            if g == 0:
                first, core = reach(chunk // 2), 1 - chunk % 2
            else:
                first, core = chunk // 2, chunk % 2
                second = reach((second // 2 + core) % 2 * 2 + second % 2)
            at = {
                order[0]: (here[order[0]] + first) % 4,
                order[1]: (here[order[1]] + second) % 4,
                order[2]: (here[order[2]] + third) % 4,
                "c": (here["c"] + core) % 2,
            }
            return at, k

        at, k = split(place)
        wanted = (((at["y"] * 4 + at["x"]) * 2 + at["c"]) * 4 + at["z"]) * 4 + k
        hits = jnp.where(wanted == slot_ref[...], 1.0, 0.0).astype(BF16)
        found = lax.dot_general(
            facts, hits, (((1,), (1,)), ((), ())), preferred_element_type=F32
        )
        if g == 0:
            index_vmem[...] = (found[0:1] + BLOCKS).astype(jnp.int32)
            index_copy.start()
        at, k = split(along)
        owner = at[STAGES[g][1]] * 4 + at[STAGES[g][2]]
        code = found[1:2] + (owner * TARGETS).astype(F32)
        for pair in range(4):
            both = code[:, pair * CELL : (pair + 1) * CELL]
            rolled = pltpu.roll(both, CHUNK, 1)
            for half in range(2 if g else 1):
                cs[half, g, 2 * pair, 0:1, :] = jnp.where(low, both, rolled)
                cs[half, g, 2 * pair + 1, 0:1, :] = jnp.where(low, rolled, both)

    fill(0)

    loads[2].wait()
    loads[3].wait()
    live = live_ref[0]

    def build(i, total):
        for j in range(8):
            block = i * 8 + j
            alive = (block < live).astype(jnp.int32)
            mask = (mask_ref[pl.ds(block, 1), :] * alive).astype(F32)
            values = fields_ref[:, pl.ds(pl.multiple_of(block * CELL, CELL), CELL)].astype(F32)
            stacked = jnp.concatenate([values * mask, jnp.broadcast_to(mask, (4, CELL))], axis=0)
            total += stacked
            stack_ref[block] = stacked.astype(BF16)
        return total

    total = lax.fori_loop(0, BLOCKS // 8, build, jnp.zeros((16, CELL), F32))
    stack_ref[BLOCKS] = jnp.zeros((16, CELL), BF16)
    t_send[0] = spread(jnp.sum(total, axis=1, keepdims=True), CELL, 0)
    fill(1)
    fill(2)
    pl.semaphore_wait(barrier, len(greeted))

    for slot in range(1, 8):
        remote(
            t_send.at[0], t1.at[slot], tsend.at[0], trecv.at[0], peer(z=slot // 2, c=slot % 2)[1]
        ).start()
    index_copy.wait()
    for copy in weight_loads:
        copy.wait()

    def products(t, core, group):
        mine = t * 2 + 1 - core
        stage = stages[core]
        results = []
        for j in range(8):
            at = mine * CHUNK + group * 8 + j
            block = jnp.clip(index_smem[0, at], 0, BLOCKS)
            results.append(
                jnp.dot(
                    stack_ref[block],
                    weights_ref[jnp.minimum(block, BLOCKS - 1)],
                    preferred_element_type=F32,
                )
            )
        for j in range(8):
            i, n = group // 2, (group % 2) * 8 + j
            value = results[j]
            stage[0][pl.ds(i * 16 + n, 4, stride=64), :] = value[0:4]
            stage[1][pl.ds(i * 64 + n, 4, stride=16), :] = value[4:8]
            stage[2][pl.ds((n // 4) * 80 + i * 4 + n % 4, 5, stride=16), :] = value[8:13]

    def code_tile(t, core, g, u, rows):
        stage = stages[core][g]
        if g == 0:
            mine = t * 2 + 1 - core
            scale = encode(
                [stage[r * 64 + u * 16 : r * 64 + u * 16 + 16, :] for r in range(4)],
                lambda r, v: q_a.__setitem__((mine, u, r), v),
            )
            rows.append(spread(scale, CHUNK, u * 16))
        else:
            base = u * ROWS[g] * 16
            slot = u * 2 + core
            scale = encode(
                [stage[base + r * 16 : base + r * 16 + 16, :] for r in range(ROWS[g])],
                lambda r, v: q[g].__setitem__((slot, t, r), v),
            )
            half = t // 2
            lane = lax.rem(half + core, 2) * 32 + lax.rem(t, 2) * 16
            cs[half, g, slot, 1:2, :] += spread(scale, CHUNK, lane)

    def ship(t, core, rows, home):
        half = t // 2
        mine = t * 2 + 1 - core
        cs[0, 0, mine, 1:2, :] = (rows[0] + rows[1]) + (rows[2] + rows[3])
        if not home:
            device = peer(z=reach(t), c=core)[1]
            remote(
                cs.at[0, 0, mine], c1.at[0, 0, mine], csend.at[0, 0], crecv.at[0, half], device
            ).start()
            remote(q_a.at[mine], r1_a.at[mine], send1.at[0], recv1.at[0, half], device).start()
        for u in (2, 1, 3, 0):
            for g in (1, 2):
                if u or core:
                    slot = u * 2 + core
                    remote(
                        q[g].at[slot, t], r1[g].at[slot, t], send1.at[g], recv1.at[g, half],
                        peer(**{STAGES[g][0]: u, "c": core})[1],
                    ).start()

    def ship_heads(half):
        for slot in range(1, 8):
            for g in (1, 2):
                remote(
                    cs.at[half, g, slot], c1.at[half, g, slot],
                    csend.at[g, half], crecv.at[g, half],
                    peer(**{STAGES[g][0]: slot // 2, "c": slot % 2})[1],
                ).start()

    tiles = [(g, u) for g in range(3) for u in range(4)]

    def together(ahead, behind, home=False):
        rows = []
        done = 0
        for group in range(8):
            if ahead is not None:
                products(*ahead, group)
            if behind is not None:
                upto = (group + 1) * len(tiles) // 8
                for g, u in tiles[done:upto]:
                    code_tile(*behind, g, u, rows)
                done = upto
        if behind is not None:
            ship(*behind, rows, home)

    together((0, 1), None)

    def step(t, carry):
        together((t, 0), (t, 1))
        together((t + 1, 1), (t, 0))

        @pl.when(t == 1)
        def _():
            ship_heads(0)

        return carry

    lax.fori_loop(0, 3, step, 0)
    together((3, 0), (3, 1))
    together(None, (3, 0), home=True)

    ship_heads(1)

    def batch(src, dst, send, recv):
        return remote(src, dst, send, recv, partner)

    rest = pl.ds(1, 7)
    sums_first = batch(t1.at[rest], t1.at[rest], tsend.at[0], trecv.at[0])
    sums_first.wait_recv()
    total = t_send[0]
    for slot in range(1, 8):
        total += t1[slot]
    t_send[1] = total
    far = sorted(range(1, 16), key=lambda n: -(min(n // 4, 4 - n // 4) + min(n % 4, 4 - n % 4)))
    for n in far:
        remote(
            t_send.at[1], t2.at[n], tsend.at[1], trecv.at[1], peer(x=n // 4, y=n % 4)[1]
        ).start()

    ends = [sums_first]
    others = pl.ds(1, 15)
    quarter = lax.broadcasted_iota(jnp.int32, (1, CELL), 1) // 32

    def combine(g, half):
        if g == 0:
            slots = list(range(4 * half, 4 * half + 4))
            n = 4 - half
            heads, datas = c1.at[0, 0, pl.ds(4 * half, n)], r1_a.at[pl.ds(4 * half, n)]
            pieces = [(slot, part) for slot in slots for part in range(4)]
            own = 7
        else:
            slots = [slot ^ half for slot in range(8)]
            heads = c1.at[half, g, rest]
            datas = r1[g].at[rest, pl.ds(2 * half, 2)]
            pieces = [(slot, 2 * half + part) for slot in slots for part in range(2)]
            own = 0
        batch(heads, heads, csend.at[g, 0], crecv.at[g, half]).wait_recv()
        batch(datas, datas, send1.at[g], recv1.at[g, half]).wait_recv()

        def lane_row(at):
            level = half if g else 0
            rows = [
                (cs if slot == own else c1)[level, g, slot, at : at + 1, :] for slot in slots
            ]
            if g == 0:
                parts = [jnp.where(low, rows[2 * p], rows[2 * p + 1]) for p in range(2)]
            else:
                parts = []
                for p in range(2):
                    a, b, c, d = rows[4 * p : 4 * p + 4]
                    parts.append(
                        jnp.where(low, jnp.where(quarter == 0, a, b), jnp.where(quarter == 2, c, d))
                    )
            return jnp.concatenate(parts, axis=1)

        targets = lax.broadcasted_iota(jnp.int32, (256, 256), 0).astype(F32)
        select = jnp.where(targets == lane_row(0), lane_row(1), 0.0).astype(BF16)
        for row in range(ROWS[g]):
            data = jnp.concatenate(
                [(q if slot == own else r1)[g][slot, part, row] for slot, part in pieces], axis=0
            )
            both = jnp.dot(select, decode(data), preferred_element_type=F32)
            both = both[:, :CELL] + both[:, CELL:]
            s2[g][row] = s2[g][row] + both if half else both

    for g in range(3):
        combine(g, 0)
    for g in range(3):
        combine(g, 1)
        for owner in range(16):
            scale = encode(
                [s2[g][r, owner * 16 : owner * 16 + 16, :] for r in range(ROWS[g])],
                lambda r, v: q2[g].__setitem__((owner, r), v),
            )
            cs2[g, owner, 0:1, :] = spread(scale, 16, 0)
        second, third = STAGES[g][1:]
        for n in far:
            at, device = peer(**{second: n // 4, third: n % 4})
            owner = at[second] * 4 + at[third]
            remote(
                cs2.at[g, owner], c2.at[g, n], c2send.at[g], c2recv.at[g], device
            ).start()
            remote(q2[g].at[owner], r2[g].at[n], send2.at[g], recv2.at[g], device).start()

    sums_second = batch(t2.at[others], t2.at[others], tsend.at[1], trecv.at[1])
    sums_second.wait_recv()
    ends.append(sums_second)
    total = t_send[1]
    for n in range(1, 16):
        total += t2[n]
    lanes = lax.broadcasted_iota(jnp.int32, (16, CELL), 1)
    rows = lax.broadcasted_iota(jnp.int32, (16, CELL), 0)
    total = jnp.sum(jnp.where(lanes == rows, total, 0.0), axis=1, keepdims=True)
    mean = total[0:12] / jnp.maximum(total[12:13], 1.0)
    group_of = lax.broadcasted_iota(jnp.int32, (1, CELL), 1) // 16
    for g in range(3):
        heads = batch(c2.at[g, others], c2.at[g, others], c2send.at[g], c2recv.at[g])
        datas = batch(r2[g].at[others], r2[g].at[others], send2.at[g], recv2.at[g])
        heads.wait_recv()
        datas.wait_recv()
        ends += [heads, datas]
        mine = here[STAGES[g][1]] * 4 + here[STAGES[g][2]]
        halves = []
        for half in range(2):
            row = jnp.zeros((1, CELL), F32)
            for n in range(8):
                source = cs2[g, mine, 0:1, :] if half + n == 0 else c2[g, half * 8 + n, 0:1, :]
                row = jnp.where(group_of == n, source, row)
            halves.append(row)
        scales = jnp.concatenate(halves, axis=1)
        rows = lax.broadcasted_iota(jnp.int32, (16, 256), 0)
        lanes = lax.broadcasted_iota(jnp.int32, (16, 256), 1) % 16
        select = jnp.where(rows == lanes, scales, 0.0).astype(BF16)
        for row in range(ROWS[g]):
            data = jnp.concatenate(
                [q2[g][mine, row]] + [r2[g][n, row] for n in range(1, 16)], axis=0
            )
            both = jnp.dot(select, decode(data), preferred_element_type=F32)
            final_ref[pl.ds((FIRST[g] + row) * TARGETS, TARGETS), :] = (
                both[:, :CELL] + both[:, CELL:]
            )
    for t in range(TARGETS):
        numer = final_ref[pl.ds(t, 12, stride=TARGETS), :]
        fraction = final_ref[pl.ds(12 * TARGETS + t, 1), :]
        filled = numer + jnp.maximum(0.25 - fraction, 0.0) * mean
        out_ref[:, t * CELL : (t + 1) * CELL] = filled / jnp.maximum(fraction, 0.25)
    for copy in ends:
        copy.wait_send()
    for g in range(3):
        mine = pl.ds(1, 7) if g else pl.ds(0, 7)
        batch(q[g].at[mine], q[g].at[mine], send1.at[g], recv1.at[g, 0]).wait_send()
        for half in range(2 if g else 1):
            heads = cs.at[half, g, mine]
            batch(heads, heads, csend.at[g, half], crecv.at[g, half]).wait_send()


def body(fields, land_mask, intersection, send_slot, target_block, live_blocks):
    smem = pl.BlockSpec(memory_space=pltpu.SMEM)
    hbm = pl.BlockSpec(memory_space=pl.ANY)
    dma = pltpu.SemaphoreType.DMA
    vmem = pltpu.VMEM
    i16 = jnp.int16
    i32 = jnp.int32
    return pl.pallas_call(
        kernel,
        in_specs=[smem] + [hbm] * 5,
        out_shape=pltpu.VMEM((12, TARGETS * CELL), F32),
        scratch_shapes=[vmem((1, BLOCKS), i32), vmem((1, BLOCKS), i32)]
        + [vmem((12, BLOCKS * CELL), BF16), vmem((BLOCKS, CELL), i32)]
        + [vmem((BLOCKS, CELL, CELL), BF16), vmem((BLOCKS + 1, 16, CELL), BF16)]
        + [vmem((1, 512), i32), pltpu.SMEM((1, 512), i32)]
        + [vmem((n, CELL), F32) for n in (576, 336, 384)] * 2
        + [vmem((8, 4, r, 16, CELL), i16) for r in ROWS] * 2
        + [vmem((2, 3, 8, 2, CELL), F32)] * 2
        + [vmem((r, 256, CELL), F32) for r in ROWS]
        + [vmem((16, r, 16, CELL), i16) for r in ROWS] * 2
        + [vmem((3, 16, 1, CELL), F32)] * 2
        + [vmem((16 * TARGETS, CELL), F32)]
        + [vmem((2, 1, CELL), F32), vmem((8, 1, CELL), F32), vmem((16, 1, CELL), F32)]
        + [dma((5,)), dma((WEIGHT_COPIES,))]
        + [dma((3,)), dma((3, 2)), dma((3, 2)), dma((3, 2))]
        + [dma((3,))] * 4
        + [dma((2,))] * 2,
        compiler_params=pltpu.CompilerParams(
            collective_id=0, has_side_effects=True, vmem_limit_bytes=62 * 1024 * 1024
        ),
        name="remap",
    )(
        live_blocks,
        send_slot.reshape(1, BLOCKS),
        target_block.reshape(1, BLOCKS),
        fields,
        land_mask.reshape(BLOCKS, CELL),
        intersection,
    )


def solution(mesh):
    axes = ("band", "sub")
    return jax.shard_map(
        body,
        mesh=mesh,
        in_specs=(P(None, axes), P(axes), P(axes, None, None), P(axes), P(axes), P(axes)),
        out_specs=P(None, axes),
        check_vma=False,
    )
```

```python
import jax
import jax.numpy as jnp
from jax import lax
from jax.experimental import pallas as pl
from jax.experimental.pallas import tpu as pltpu
from jax.sharding import PartitionSpec as P

CELL = 128
BLOCKS = 256
TARGETS = 16
CHUNK = 64
ROWS = (4, 4, 5)
FIRST = (0, 4, 8)
STAGES = ("zxy", "xyz", "yzx")
SLOTS = ("zxy", "xzy", "yzx")
MESH = pl.DeviceIdType.MESH
F32 = jnp.float32
BF16 = jnp.bfloat16
WEIGHT_COPIES = 1


def encode(tiles, write):
    top = jnp.abs(tiles[0])
    for tile in tiles[1:]:
        top = jnp.maximum(top, jnp.abs(tile))
    top = jnp.maximum(jnp.max(top, axis=1, keepdims=True), 1e-25)
    power = jnp.ceil(jnp.log2(top) + 0.02)
    down = jnp.exp2(-power)
    for row, tile in enumerate(tiles):
        small = tile * down
        code = small * lax.rsqrt(jnp.abs(small) + 1e-30) * 32768.0
        write(row, jnp.round(code).astype(jnp.int32).astype(jnp.int16))
    return jnp.exp2(power - 30.0)


def spread(scale, period, lane):
    lanes = lax.broadcasted_iota(jnp.int32, (16, CELL), 1) % period
    slots = lax.broadcasted_iota(jnp.int32, (16, CELL), 0) + lane
    return jnp.sum(jnp.where(lanes == slots, scale, 0.0), axis=0, keepdims=True)


def decode(codes):
    value = codes.astype(F32)
    value = value * jnp.abs(value)
    high = value.astype(BF16)
    return jnp.concatenate([high, (value - high.astype(F32)).astype(BF16)], axis=1)


def kernel(
    live_ref, slot_hbm, target_hbm, fields_hbm, mask_hbm, weights_hbm, out_ref,
    slot_ref, target_ref, fields_ref, mask_ref, weights_ref, stack_ref, index_vmem, index_smem,
    even_a, even_b, even_c, odd_a, odd_b, odd_c, q_a, q_b, q_c, r1_a, r1_b, r1_c, cs, c1,
    s2_a, s2_b, s2_c, q2_a, q2_b, q2_c, r2_a, r2_b, r2_c, cs2, c2, final_ref, t_send, t1, t2,
    load, wload, send1, recv1, csend, crecv, send2, recv2, c2send, c2recv, tsend, trecv,
):
    stages = ((even_a, even_b, even_c), (odd_a, odd_b, odd_c))
    q = (q_a, q_b, q_c)
    r1 = (r1_a, r1_b, r1_c)
    s2 = (s2_a, s2_b, s2_c)
    q2 = (q2_a, q2_b, q2_c)
    r2 = (r2_a, r2_b, r2_c)
    band = lax.axis_index("band")
    here = {
        "y": band // 8,
        "x": lax.rem(band // 2, 4),
        "c": lax.rem(band, 2),
        "z": lax.axis_index("sub"),
    }

    def peer(**shifts):
        at = {}
        for dim in "yxcz":
            at[dim] = here[dim]
            if dim in shifts:
                at[dim] = lax.rem(here[dim] + shifts[dim], 2 if dim == "c" else 4)
        return at, ((at["y"] * 4 + at["x"]) * 2 + at["c"], at["z"])

    def remote(src, dst, send, recv, device):
        return pltpu.make_async_remote_copy(
            src_ref=src, dst_ref=dst, send_sem=send, recv_sem=recv,
            device_id=device, device_id_type=MESH,
        )

    partner = peer(c=1)[1]

    def reach(t):
        near = 1 + 2 * here["c"]
        return jnp.where(t == 0, 2, jnp.where(t == 1, near, jnp.where(t == 2, 4 - near, 0)))

    loads = [
        pltpu.make_async_copy(slot_hbm, slot_ref, load.at[0]),
        pltpu.make_async_copy(target_hbm, target_ref, load.at[1]),
        pltpu.make_async_copy(mask_hbm, mask_ref, load.at[2]),
        pltpu.make_async_copy(fields_hbm, fields_ref, load.at[3]),
    ]
    size = BLOCKS // WEIGHT_COPIES
    weight_loads = [
        pltpu.make_async_copy(
            weights_hbm.at[pl.ds(i * size, size)], weights_ref.at[pl.ds(i * size, size)], wload.at[i]
        )
        for i in range(WEIGHT_COPIES)
    ]
    for copy in loads + weight_loads:
        copy.start()

    barrier = pltpu.get_barrier_semaphore()
    greeted = set()
    for g in range(3):
        for n in range(1, 8):
            greeted.add(tuple(sorted({STAGES[g][0]: n // 2, "c": n % 2}.items())))
    greeted = {tuple(item for item in names if item[1]) for names in greeted}
    for names in sorted(greeted):
        pl.semaphore_signal(
            barrier, inc=1, device_id=peer(**dict(names))[1], device_id_type=MESH
        )

    low = lax.broadcasted_iota(jnp.int32, (1, CELL), 1) < CHUNK
    blocks = lax.broadcasted_iota(jnp.int32, (8, BLOCKS), 1)
    kind = lax.broadcasted_iota(jnp.int32, (8, BLOCKS), 0)
    place = lax.broadcasted_iota(jnp.int32, (512, 1), 0)
    along = lax.broadcasted_iota(jnp.int32, (1, 512), 1)
    cs[...] = jnp.zeros_like(cs)
    loads[0].wait()
    loads[1].wait()
    facts = jnp.where(kind == 0, blocks - BLOCKS, jnp.broadcast_to(target_ref[...], (8, BLOCKS)))
    facts = facts.astype(F32).astype(BF16)
    index_copy = pltpu.make_async_copy(index_vmem, index_smem, load.at[4])

    def fill(g):
        order = SLOTS[g]

        def split(n):
            chunk, second, third, k = n // 64, (n // 16) % 4, (n // 4) % 4, n % 4
            if g == 0:
                first, core = reach(chunk // 2), 1 - chunk % 2
            else:
                first, core = chunk // 2, chunk % 2
                second = reach((second // 2 + core) % 2 * 2 + second % 2)
            at = {
                order[0]: (here[order[0]] + first) % 4,
                order[1]: (here[order[1]] + second) % 4,
                order[2]: (here[order[2]] + third) % 4,
                "c": (here["c"] + core) % 2,
            }
            return at, k

        at, k = split(place)
        wanted = (((at["y"] * 4 + at["x"]) * 2 + at["c"]) * 4 + at["z"]) * 4 + k
        hits = jnp.where(wanted == slot_ref[...], 1.0, 0.0).astype(BF16)
        found = lax.dot_general(
            facts, hits, (((1,), (1,)), ((), ())), preferred_element_type=F32
        )
        if g == 0:
            index_vmem[...] = (found[0:1] + BLOCKS).astype(jnp.int32)
            index_copy.start()
        at, k = split(along)
        owner = at[STAGES[g][1]] * 4 + at[STAGES[g][2]]
        code = found[1:2] + (owner * TARGETS).astype(F32)
        for pair in range(4):
            both = code[:, pair * CELL : (pair + 1) * CELL]
            rolled = pltpu.roll(both, CHUNK, 1)
            for half in range(2 if g else 1):
                cs[half, g, 2 * pair, 0:1, :] = jnp.where(low, both, rolled)
                cs[half, g, 2 * pair + 1, 0:1, :] = jnp.where(low, rolled, both)

    fill(0)

    loads[2].wait()
    loads[3].wait()
    live = live_ref[0]

    def build(i, total):
        for j in range(8):
            block = i * 8 + j
            alive = (block < live).astype(jnp.int32)
            mask = (mask_ref[pl.ds(block, 1), :] * alive).astype(F32)
            values = fields_ref[:, pl.ds(pl.multiple_of(block * CELL, CELL), CELL)].astype(F32)
            stacked = jnp.concatenate([values * mask, jnp.broadcast_to(mask, (4, CELL))], axis=0)
            total += stacked
            stack_ref[block] = stacked.astype(BF16)
        return total

    total = lax.fori_loop(0, BLOCKS // 8, build, jnp.zeros((16, CELL), F32))
    stack_ref[BLOCKS] = jnp.zeros((16, CELL), BF16)
    t_send[0] = spread(jnp.sum(total, axis=1, keepdims=True), CELL, 0)
    fill(1)
    fill(2)
    pl.semaphore_wait(barrier, len(greeted))

    for slot in range(1, 8):
        remote(
            t_send.at[0], t1.at[slot], tsend.at[0], trecv.at[0], peer(z=slot // 2, c=slot % 2)[1]
        ).start()
    index_copy.wait()
    for copy in weight_loads:
        copy.wait()

    def products(t, core, group):
        mine = t * 2 + 1 - core
        stage = stages[core]
        results = []
        for j in range(8):
            at = mine * CHUNK + group * 8 + j
            block = jnp.clip(index_smem[0, at], 0, BLOCKS)
            results.append(
                jnp.dot(
                    stack_ref[block],
                    weights_ref[jnp.minimum(block, BLOCKS - 1)],
                    preferred_element_type=F32,
                )
            )
        for j in range(8):
            i, n = group // 2, (group % 2) * 8 + j
            value = results[j]
            stage[0][pl.ds(i * 16 + n, 4, stride=64), :] = value[0:4]
            stage[1][pl.ds(i * 64 + n, 4, stride=16), :] = value[4:8]
            stage[2][pl.ds((n // 4) * 80 + i * 4 + n % 4, 5, stride=16), :] = value[8:13]

    def code_tile(t, core, g, u, rows):
        stage = stages[core][g]
        if g == 0:
            mine = t * 2 + 1 - core
            scale = encode(
                [stage[r * 64 + u * 16 : r * 64 + u * 16 + 16, :] for r in range(4)],
                lambda r, v: q_a.__setitem__((mine, u, r), v),
            )
            rows.append(spread(scale, CHUNK, u * 16))
        else:
            base = u * ROWS[g] * 16
            slot = u * 2 + core
            scale = encode(
                [stage[base + r * 16 : base + r * 16 + 16, :] for r in range(ROWS[g])],
                lambda r, v: q[g].__setitem__((slot, t, r), v),
            )
            half = t // 2
            lane = lax.rem(half + core, 2) * 32 + lax.rem(t, 2) * 16
            cs[half, g, slot, 1:2, :] += spread(scale, CHUNK, lane)

    def ship(t, core, rows, home):
        half = t // 2
        mine = t * 2 + 1 - core
        cs[0, 0, mine, 1:2, :] = (rows[0] + rows[1]) + (rows[2] + rows[3])
        if not home:
            device = peer(z=reach(t), c=core)[1]
            remote(
                cs.at[0, 0, mine], c1.at[0, 0, mine], csend.at[0, 0], crecv.at[0, half], device
            ).start()
            remote(q_a.at[mine], r1_a.at[mine], send1.at[0], recv1.at[0, half], device).start()
        for u in (2, 1, 3, 0):
            for g in (1, 2):
                if u or core:
                    slot = u * 2 + core
                    remote(
                        q[g].at[slot, t], r1[g].at[slot, t], send1.at[g], recv1.at[g, half],
                        peer(**{STAGES[g][0]: u, "c": core})[1],
                    ).start()

    def ship_heads(half):
        for slot in range(1, 8):
            for g in (1, 2):
                remote(
                    cs.at[half, g, slot], c1.at[half, g, slot],
                    csend.at[g, half], crecv.at[g, half],
                    peer(**{STAGES[g][0]: slot // 2, "c": slot % 2})[1],
                ).start()

    tiles = [(g, u) for g in range(3) for u in range(4)]

    def together(ahead, behind, home=False):
        rows = []
        done = 0
        for group in range(8):
            if ahead is not None:
                products(*ahead, group)
            if behind is not None:
                upto = (group + 1) * len(tiles) // 8
                for g, u in tiles[done:upto]:
                    code_tile(*behind, g, u, rows)
                done = upto
        if behind is not None:
            ship(*behind, rows, home)

    together((0, 1), None)

    def step(t, carry):
        together((t, 0), (t, 1))
        together((t + 1, 1), (t, 0))

        @pl.when(t == 1)
        def _():
            ship_heads(0)

        return carry

    lax.fori_loop(0, 3, step, 0)
    together((3, 0), (3, 1))
    together(None, (3, 0), home=True)

    ship_heads(1)

    def batch(src, dst, send, recv):
        return remote(src, dst, send, recv, partner)

    rest = pl.ds(1, 7)
    sums_first = batch(t1.at[rest], t1.at[rest], tsend.at[0], trecv.at[0])
    far = sorted(range(1, 16), key=lambda n: -(min(n // 4, 4 - n // 4) + min(n % 4, 4 - n % 4)))
    ends = [sums_first]
    others = pl.ds(1, 15)
    quarter = lax.broadcasted_iota(jnp.int32, (1, CELL), 1) // 32

    def combine(g, half):
        if g == 0:
            slots = list(range(4 * half, 4 * half + 4))
            n = 4 - half
            heads, datas = c1.at[0, 0, pl.ds(4 * half, n)], r1_a.at[pl.ds(4 * half, n)]
            pieces = [(slot, part) for slot in slots for part in range(4)]
            own = 7
        else:
            slots = [slot ^ half for slot in range(8)]
            heads = c1.at[half, g, rest]
            datas = r1[g].at[rest, pl.ds(2 * half, 2)]
            pieces = [(slot, 2 * half + part) for slot in slots for part in range(2)]
            own = 0
        batch(heads, heads, csend.at[g, 0], crecv.at[g, half]).wait_recv()
        batch(datas, datas, send1.at[g], recv1.at[g, half]).wait_recv()

        def lane_row(at):
            level = half if g else 0
            rows = [
                (cs if slot == own else c1)[level, g, slot, at : at + 1, :] for slot in slots
            ]
            if g == 0:
                parts = [jnp.where(low, rows[2 * p], rows[2 * p + 1]) for p in range(2)]
            else:
                parts = []
                for p in range(2):
                    a, b, c, d = rows[4 * p : 4 * p + 4]
                    parts.append(
                        jnp.where(low, jnp.where(quarter == 0, a, b), jnp.where(quarter == 2, c, d))
                    )
            return jnp.concatenate(parts, axis=1)

        targets = lax.broadcasted_iota(jnp.int32, (256, 256), 0).astype(F32)
        select = jnp.where(targets == lane_row(0), lane_row(1), 0.0).astype(BF16)
        for row in range(ROWS[g]):
            data = jnp.concatenate(
                [(q if slot == own else r1)[g][slot, part, row] for slot, part in pieces], axis=0
            )
            both = jnp.dot(select, decode(data), preferred_element_type=F32)
            both = both[:, :CELL] + both[:, CELL:]
            s2[g][row] = s2[g][row] + both if half else both

    for g in (1, 2, 0):
        if g == 0:
            sums_first.wait_recv()
            total = t_send[0]
            for slot in range(1, 8):
                total += t1[slot]
            t_send[1] = total
            for n in far:
                remote(
                    t_send.at[1], t2.at[n], tsend.at[1], trecv.at[1], peer(x=n // 4, y=n % 4)[1]
                ).start()
        for other in {1: (1, 2), 2: (), 0: (0,)}[g]:
            combine(other, 0)
        combine(g, 1)
        for owner in range(16):
            scale = encode(
                [s2[g][r, owner * 16 : owner * 16 + 16, :] for r in range(ROWS[g])],
                lambda r, v: q2[g].__setitem__((owner, r), v),
            )
            cs2[g, owner, 0:1, :] = spread(scale, 16, 0)
        second, third = STAGES[g][1:]
        for n in far:
            at, device = peer(**{second: n // 4, third: n % 4})
            owner = at[second] * 4 + at[third]
            remote(
                cs2.at[g, owner], c2.at[g, n], c2send.at[g], c2recv.at[g], device
            ).start()
            remote(q2[g].at[owner], r2[g].at[n], send2.at[g], recv2.at[g], device).start()

    sums_second = batch(t2.at[others], t2.at[others], tsend.at[1], trecv.at[1])
    sums_second.wait_recv()
    ends.append(sums_second)
    total = t_send[1]
    for n in range(1, 16):
        total += t2[n]
    lanes = lax.broadcasted_iota(jnp.int32, (16, CELL), 1)
    rows = lax.broadcasted_iota(jnp.int32, (16, CELL), 0)
    total = jnp.sum(jnp.where(lanes == rows, total, 0.0), axis=1, keepdims=True)
    mean = total[0:12] / jnp.maximum(total[12:13], 1.0)
    group_of = lax.broadcasted_iota(jnp.int32, (1, CELL), 1) // 16
    for g in (1, 2, 0):
        heads = batch(c2.at[g, others], c2.at[g, others], c2send.at[g], c2recv.at[g])
        datas = batch(r2[g].at[others], r2[g].at[others], send2.at[g], recv2.at[g])
        heads.wait_recv()
        datas.wait_recv()
        ends += [heads, datas]
        mine = here[STAGES[g][1]] * 4 + here[STAGES[g][2]]
        halves = []
        for half in range(2):
            row = jnp.zeros((1, CELL), F32)
            for n in range(8):
                source = cs2[g, mine, 0:1, :] if half + n == 0 else c2[g, half * 8 + n, 0:1, :]
                row = jnp.where(group_of == n, source, row)
            halves.append(row)
        scales = jnp.concatenate(halves, axis=1)
        rows = lax.broadcasted_iota(jnp.int32, (16, 256), 0)
        lanes = lax.broadcasted_iota(jnp.int32, (16, 256), 1) % 16
        select = jnp.where(rows == lanes, scales, 0.0).astype(BF16)
        for row in range(ROWS[g]):
            data = jnp.concatenate(
                [q2[g][mine, row]] + [r2[g][n, row] for n in range(1, 16)], axis=0
            )
            both = jnp.dot(select, decode(data), preferred_element_type=F32)
            final_ref[pl.ds((FIRST[g] + row) * TARGETS, TARGETS), :] = (
                both[:, :CELL] + both[:, CELL:]
            )
    for t in range(TARGETS):
        numer = final_ref[pl.ds(t, 12, stride=TARGETS), :]
        fraction = final_ref[pl.ds(12 * TARGETS + t, 1), :]
        filled = numer + jnp.maximum(0.25 - fraction, 0.0) * mean
        out_ref[:, t * CELL : (t + 1) * CELL] = filled / jnp.maximum(fraction, 0.25)
    for copy in ends:
        copy.wait_send()
    for g in range(3):
        mine = pl.ds(1, 7) if g else pl.ds(0, 7)
        batch(q[g].at[mine], q[g].at[mine], send1.at[g], recv1.at[g, 0]).wait_send()
        for half in range(2 if g else 1):
            heads = cs.at[half, g, mine]
            batch(heads, heads, csend.at[g, half], crecv.at[g, half]).wait_send()


def body(fields, land_mask, intersection, send_slot, target_block, live_blocks):
    smem = pl.BlockSpec(memory_space=pltpu.SMEM)
    hbm = pl.BlockSpec(memory_space=pl.ANY)
    dma = pltpu.SemaphoreType.DMA
    vmem = pltpu.VMEM
    i16 = jnp.int16
    i32 = jnp.int32
    return pl.pallas_call(
        kernel,
        in_specs=[smem] + [hbm] * 5,
        out_shape=pltpu.VMEM((12, TARGETS * CELL), F32),
        scratch_shapes=[vmem((1, BLOCKS), i32), vmem((1, BLOCKS), i32)]
        + [vmem((12, BLOCKS * CELL), BF16), vmem((BLOCKS, CELL), i32)]
        + [vmem((BLOCKS, CELL, CELL), BF16), vmem((BLOCKS + 1, 16, CELL), BF16)]
        + [vmem((1, 512), i32), pltpu.SMEM((1, 512), i32)]
        + [vmem((n, CELL), F32) for n in (576, 336, 384)] * 2
        + [vmem((8, 4, r, 16, CELL), i16) for r in ROWS] * 2
        + [vmem((2, 3, 8, 2, CELL), F32)] * 2
        + [vmem((r, 256, CELL), F32) for r in ROWS]
        + [vmem((16, r, 16, CELL), i16) for r in ROWS] * 2
        + [vmem((3, 16, 1, CELL), F32)] * 2
        + [vmem((16 * TARGETS, CELL), F32)]
        + [vmem((2, 1, CELL), F32), vmem((8, 1, CELL), F32), vmem((16, 1, CELL), F32)]
        + [dma((5,)), dma((WEIGHT_COPIES,))]
        + [dma((3,)), dma((3, 2)), dma((3, 2)), dma((3, 2))]
        + [dma((3,))] * 4
        + [dma((2,))] * 2,
        compiler_params=pltpu.CompilerParams(
            collective_id=0, has_side_effects=True, vmem_limit_bytes=62 * 1024 * 1024
        ),
        name="remap",
    )(
        live_blocks,
        send_slot.reshape(1, BLOCKS),
        target_block.reshape(1, BLOCKS),
        fields,
        land_mask.reshape(BLOCKS, CELL),
        intersection,
    )


def solution(mesh):
    axes = ("band", "sub")
    return jax.shard_map(
        body,
        mesh=mesh,
        in_specs=(P(None, axes), P(axes), P(axes, None, None), P(axes), P(axes), P(axes)),
        out_specs=P(None, axes),
        check_vma=False,
    )
```

```python
import jax
import jax.numpy as jnp
from jax import lax
from jax.experimental import pallas as pl
from jax.experimental.pallas import tpu as pltpu
from jax.sharding import PartitionSpec as P

CELL = 128
BLOCKS = 256
TARGETS = 16
CHUNK = 64
ROWS = (5, 4, 4)
FIRST = (0, 5, 9)
STAGES = ("zxy", "xyz", "yzx")
SLOTS = ("zxy", "xzy", "yzx")
MESH = pl.DeviceIdType.MESH
F32 = jnp.float32
BF16 = jnp.bfloat16
WEIGHT_COPIES = 1


def encode(tiles, write):
    top = jnp.abs(tiles[0])
    for tile in tiles[1:]:
        top = jnp.maximum(top, jnp.abs(tile))
    top = jnp.maximum(jnp.max(top, axis=1, keepdims=True), 1e-25)
    power = jnp.ceil(jnp.log2(top) + 0.02)
    down = jnp.exp2(-power)
    for row, tile in enumerate(tiles):
        small = tile * down
        code = small * lax.rsqrt(jnp.abs(small) + 1e-30) * 32768.0
        write(row, jnp.round(code).astype(jnp.int32).astype(jnp.int16))
    return jnp.exp2(power - 30.0)


def spread(scale, period, lane):
    lanes = lax.broadcasted_iota(jnp.int32, (16, CELL), 1) % period
    slots = lax.broadcasted_iota(jnp.int32, (16, CELL), 0) + lane
    return jnp.sum(jnp.where(lanes == slots, scale, 0.0), axis=0, keepdims=True)


def decode(codes):
    value = codes.astype(F32)
    value = value * jnp.abs(value)
    high = value.astype(BF16)
    return jnp.concatenate([high, (value - high.astype(F32)).astype(BF16)], axis=1)


def kernel(
    live_ref, slot_hbm, target_hbm, fields_hbm, mask_hbm, weights_hbm, out_ref,
    slot_ref, target_ref, fields_ref, mask_ref, weights_ref, stack_ref, index_vmem, index_smem,
    even_a, even_b, even_c, odd_a, odd_b, odd_c, q_a, q_b, q_c, r1_a, r1_b, r1_c, cs, c1,
    s2_a, s2_b, s2_c, q2_a, q2_b, q2_c, r2_a, r2_b, r2_c, cs2, c2, final_ref, t_send, t1, t2,
    load, wload, send1, recv1, csend, crecv, send2, recv2, c2send, c2recv, tsend, trecv,
):
    stages = ((even_a, even_b, even_c), (odd_a, odd_b, odd_c))
    q = (q_a, q_b, q_c)
    r1 = (r1_a, r1_b, r1_c)
    s2 = (s2_a, s2_b, s2_c)
    q2 = (q2_a, q2_b, q2_c)
    r2 = (r2_a, r2_b, r2_c)
    band = lax.axis_index("band")
    here = {
        "y": band // 8,
        "x": lax.rem(band // 2, 4),
        "c": lax.rem(band, 2),
        "z": lax.axis_index("sub"),
    }

    def peer(**shifts):
        at = {}
        for dim in "yxcz":
            at[dim] = here[dim]
            if dim in shifts:
                at[dim] = lax.rem(here[dim] + shifts[dim], 2 if dim == "c" else 4)
        return at, ((at["y"] * 4 + at["x"]) * 2 + at["c"], at["z"])

    def remote(src, dst, send, recv, device):
        return pltpu.make_async_remote_copy(
            src_ref=src, dst_ref=dst, send_sem=send, recv_sem=recv,
            device_id=device, device_id_type=MESH,
        )

    partner = peer(c=1)[1]

    def reach(t):
        near = 1 + 2 * here["c"]
        return jnp.where(t == 0, 2, jnp.where(t == 1, near, jnp.where(t == 2, 4 - near, 0)))

    loads = [
        pltpu.make_async_copy(slot_hbm, slot_ref, load.at[0]),
        pltpu.make_async_copy(target_hbm, target_ref, load.at[1]),
        pltpu.make_async_copy(mask_hbm, mask_ref, load.at[2]),
        pltpu.make_async_copy(fields_hbm, fields_ref, load.at[3]),
    ]
    size = BLOCKS // WEIGHT_COPIES
    weight_loads = [
        pltpu.make_async_copy(
            weights_hbm.at[pl.ds(i * size, size)], weights_ref.at[pl.ds(i * size, size)], wload.at[i]
        )
        for i in range(WEIGHT_COPIES)
    ]
    for copy in loads + weight_loads:
        copy.start()

    barrier = pltpu.get_barrier_semaphore()
    greeted = set()
    for g in range(3):
        for n in range(1, 8):
            greeted.add(tuple(sorted({STAGES[g][0]: n // 2, "c": n % 2}.items())))
    greeted = {tuple(item for item in names if item[1]) for names in greeted}
    for names in sorted(greeted):
        pl.semaphore_signal(
            barrier, inc=1, device_id=peer(**dict(names))[1], device_id_type=MESH
        )

    low = lax.broadcasted_iota(jnp.int32, (1, CELL), 1) < CHUNK
    blocks = lax.broadcasted_iota(jnp.int32, (8, BLOCKS), 1)
    kind = lax.broadcasted_iota(jnp.int32, (8, BLOCKS), 0)
    place = lax.broadcasted_iota(jnp.int32, (512, 1), 0)
    along = lax.broadcasted_iota(jnp.int32, (1, 512), 1)
    cs[...] = jnp.zeros_like(cs)
    loads[0].wait()
    loads[1].wait()
    facts = jnp.where(kind == 0, blocks - BLOCKS, jnp.broadcast_to(target_ref[...], (8, BLOCKS)))
    facts = facts.astype(F32).astype(BF16)
    index_copy = pltpu.make_async_copy(index_vmem, index_smem, load.at[4])

    def fill(g):
        order = SLOTS[g]

        def split(n):
            chunk, second, third, k = n // 64, (n // 16) % 4, (n // 4) % 4, n % 4
            if g == 0:
                first, core = reach(chunk // 2), 1 - chunk % 2
            else:
                first, core = chunk // 2, chunk % 2
                second = reach((second // 2 + core) % 2 * 2 + second % 2)
            at = {
                order[0]: (here[order[0]] + first) % 4,
                order[1]: (here[order[1]] + second) % 4,
                order[2]: (here[order[2]] + third) % 4,
                "c": (here["c"] + core) % 2,
            }
            return at, k

        at, k = split(place)
        wanted = (((at["y"] * 4 + at["x"]) * 2 + at["c"]) * 4 + at["z"]) * 4 + k
        hits = jnp.where(wanted == slot_ref[...], 1.0, 0.0).astype(BF16)
        found = lax.dot_general(
            facts, hits, (((1,), (1,)), ((), ())), preferred_element_type=F32
        )
        if g == 0:
            index_vmem[...] = (found[0:1] + BLOCKS).astype(jnp.int32)
            index_copy.start()
        at, k = split(along)
        owner = at[STAGES[g][1]] * 4 + at[STAGES[g][2]]
        code = found[1:2] + (owner * TARGETS).astype(F32)
        for pair in range(4):
            both = code[:, pair * CELL : (pair + 1) * CELL]
            rolled = pltpu.roll(both, CHUNK, 1)
            for half in range(2 if g else 1):
                cs[half, g, 2 * pair, 0:1, :] = jnp.where(low, both, rolled)
                cs[half, g, 2 * pair + 1, 0:1, :] = jnp.where(low, rolled, both)

    fill(0)

    loads[2].wait()
    loads[3].wait()
    live = live_ref[0]

    def build(i, total):
        for j in range(8):
            block = i * 8 + j
            alive = (block < live).astype(jnp.int32)
            mask = (mask_ref[pl.ds(block, 1), :] * alive).astype(F32)
            values = fields_ref[:, pl.ds(pl.multiple_of(block * CELL, CELL), CELL)].astype(F32)
            stacked = jnp.concatenate([values * mask, jnp.broadcast_to(mask, (4, CELL))], axis=0)
            total += stacked
            stack_ref[block] = stacked.astype(BF16)
        return total

    total = lax.fori_loop(0, BLOCKS // 8, build, jnp.zeros((16, CELL), F32))
    stack_ref[BLOCKS] = jnp.zeros((16, CELL), BF16)
    t_send[0] = spread(jnp.sum(total, axis=1, keepdims=True), CELL, 0)
    fill(1)
    fill(2)
    pl.semaphore_wait(barrier, len(greeted))

    for slot in range(1, 8):
        remote(
            t_send.at[0], t1.at[slot], tsend.at[0], trecv.at[0], peer(z=slot // 2, c=slot % 2)[1]
        ).start()
    index_copy.wait()
    for copy in weight_loads:
        copy.wait()

    def products(t, core, group):
        mine = t * 2 + 1 - core
        stage = stages[core]
        results = []
        for j in range(8):
            at = mine * CHUNK + group * 8 + j
            block = jnp.clip(index_smem[0, at], 0, BLOCKS)
            results.append(
                jnp.dot(
                    stack_ref[block],
                    weights_ref[jnp.minimum(block, BLOCKS - 1)],
                    preferred_element_type=F32,
                )
            )
        for j in range(8):
            i, n = group // 2, (group % 2) * 8 + j
            value = results[j]
            starts = (
                i * 16 + n,
                i * ROWS[1] * 16 + n,
                (n // 4) * ROWS[2] * 16 + i * 4 + n % 4,
            )
            for g in range(3):
                part = value[FIRST[g] : FIRST[g] + ROWS[g]]
                stage[g][pl.ds(starts[g], ROWS[g], stride=16 if g else 64), :] = part

    def code_tile(t, core, g, u, rows):
        stage = stages[core][g]
        if g == 0:
            mine = t * 2 + 1 - core
            scale = encode(
                [stage[r * 64 + u * 16 : r * 64 + u * 16 + 16, :] for r in range(ROWS[0])],
                lambda r, v: q_a.__setitem__((mine, u, r), v),
            )
            rows.append(spread(scale, CHUNK, u * 16))
        else:
            base = u * ROWS[g] * 16
            slot = u * 2 + core
            scale = encode(
                [stage[base + r * 16 : base + r * 16 + 16, :] for r in range(ROWS[g])],
                lambda r, v: q[g].__setitem__((slot, t, r), v),
            )
            half = t // 2
            lane = lax.rem(half + core, 2) * 32 + lax.rem(t, 2) * 16
            cs[half, g, slot, 1:2, :] += spread(scale, CHUNK, lane)

    def ship(t, core, rows, home):
        half = t // 2
        mine = t * 2 + 1 - core
        cs[0, 0, mine, 1:2, :] = (rows[0] + rows[1]) + (rows[2] + rows[3])
        if not home:
            device = peer(z=reach(t), c=core)[1]
            remote(
                cs.at[0, 0, mine], c1.at[0, 0, mine], csend.at[0, 0], crecv.at[0, half], device
            ).start()
            remote(q_a.at[mine], r1_a.at[mine], send1.at[0], recv1.at[0, half], device).start()
        for u in (2, 1, 3, 0):
            for g in (1, 2):
                if u or core:
                    slot = u * 2 + core
                    remote(
                        q[g].at[slot, t], r1[g].at[slot, t], send1.at[g], recv1.at[g, half],
                        peer(**{STAGES[g][0]: u, "c": core})[1],
                    ).start()

    def ship_heads(half):
        for slot in range(1, 8):
            for g in (1, 2):
                remote(
                    cs.at[half, g, slot], c1.at[half, g, slot],
                    csend.at[g, half], crecv.at[g, half],
                    peer(**{STAGES[g][0]: slot // 2, "c": slot % 2})[1],
                ).start()

    tiles = [(g, u) for g in range(3) for u in range(4)]

    def together(ahead, behind, home=False):
        rows = []
        done = 0
        for group in range(8):
            if ahead is not None:
                products(*ahead, group)
            if behind is not None:
                upto = (group + 1) * len(tiles) // 8
                for g, u in tiles[done:upto]:
                    code_tile(*behind, g, u, rows)
                done = upto
        if behind is not None:
            ship(*behind, rows, home)

    together((0, 1), None)

    def step(t, carry):
        together((t, 0), (t, 1))
        together((t + 1, 1), (t, 0))

        @pl.when(t == 1)
        def _():
            ship_heads(0)

        return carry

    lax.fori_loop(0, 3, step, 0)
    together((3, 0), (3, 1))
    together(None, (3, 0), home=True)

    ship_heads(1)

    def batch(src, dst, send, recv):
        return remote(src, dst, send, recv, partner)

    rest = pl.ds(1, 7)
    sums_first = batch(t1.at[rest], t1.at[rest], tsend.at[0], trecv.at[0])
    far = sorted(range(1, 16), key=lambda n: -(min(n // 4, 4 - n // 4) + min(n % 4, 4 - n % 4)))
    ends = [sums_first]
    others = pl.ds(1, 15)
    quarter = lax.broadcasted_iota(jnp.int32, (1, CELL), 1) // 32

    def combine(g, half):
        if g == 0:
            slots = list(range(4 * half, 4 * half + 4))
            n = 4 - half
            heads, datas = c1.at[0, 0, pl.ds(4 * half, n)], r1_a.at[pl.ds(4 * half, n)]
            pieces = [(slot, part) for slot in slots for part in range(4)]
            own = 7
        else:
            slots = [slot ^ half for slot in range(8)]
            heads = c1.at[half, g, rest]
            datas = r1[g].at[rest, pl.ds(2 * half, 2)]
            pieces = [(slot, 2 * half + part) for slot in slots for part in range(2)]
            own = 0
        batch(heads, heads, csend.at[g, 0], crecv.at[g, half]).wait_recv()
        batch(datas, datas, send1.at[g], recv1.at[g, half]).wait_recv()

        def lane_row(at):
            level = half if g else 0
            rows = [
                (cs if slot == own else c1)[level, g, slot, at : at + 1, :] for slot in slots
            ]
            if g == 0:
                parts = [jnp.where(low, rows[2 * p], rows[2 * p + 1]) for p in range(2)]
            else:
                parts = []
                for p in range(2):
                    a, b, c, d = rows[4 * p : 4 * p + 4]
                    parts.append(
                        jnp.where(low, jnp.where(quarter == 0, a, b), jnp.where(quarter == 2, c, d))
                    )
            return jnp.concatenate(parts, axis=1)

        targets = lax.broadcasted_iota(jnp.int32, (256, 256), 0).astype(F32)
        select = jnp.where(targets == lane_row(0), lane_row(1), 0.0).astype(BF16)
        for row in range(ROWS[g]):
            data = jnp.concatenate(
                [(q if slot == own else r1)[g][slot, part, row] for slot, part in pieces], axis=0
            )
            both = jnp.dot(select, decode(data), preferred_element_type=F32)
            both = both[:, :CELL] + both[:, CELL:]
            s2[g][row] = s2[g][row] + both if half else both

    for g in (1, 2, 0):
        if g == 0:
            sums_first.wait_recv()
            total = t_send[0]
            for slot in range(1, 8):
                total += t1[slot]
            t_send[1] = total
            for n in far:
                remote(
                    t_send.at[1], t2.at[n], tsend.at[1], trecv.at[1], peer(x=n // 4, y=n % 4)[1]
                ).start()
        for other in {1: (1, 2), 2: (), 0: (0,)}[g]:
            combine(other, 0)
        combine(g, 1)
        for owner in range(16):
            scale = encode(
                [s2[g][r, owner * 16 : owner * 16 + 16, :] for r in range(ROWS[g])],
                lambda r, v: q2[g].__setitem__((owner, r), v),
            )
            cs2[g, owner, 0:1, :] = spread(scale, 16, 0)
        second, third = STAGES[g][1:]
        for n in far:
            at, device = peer(**{second: n // 4, third: n % 4})
            owner = at[second] * 4 + at[third]
            remote(
                cs2.at[g, owner], c2.at[g, n], c2send.at[g], c2recv.at[g], device
            ).start()
            remote(q2[g].at[owner], r2[g].at[n], send2.at[g], recv2.at[g], device).start()

    sums_second = batch(t2.at[others], t2.at[others], tsend.at[1], trecv.at[1])
    sums_second.wait_recv()
    ends.append(sums_second)
    total = t_send[1]
    for n in range(1, 16):
        total += t2[n]
    lanes = lax.broadcasted_iota(jnp.int32, (16, CELL), 1)
    rows = lax.broadcasted_iota(jnp.int32, (16, CELL), 0)
    total = jnp.sum(jnp.where(lanes == rows, total, 0.0), axis=1, keepdims=True)
    mean = total[0:12] / jnp.maximum(total[12:13], 1.0)
    group_of = lax.broadcasted_iota(jnp.int32, (1, CELL), 1) // 16
    for g in (1, 2, 0):
        heads = batch(c2.at[g, others], c2.at[g, others], c2send.at[g], c2recv.at[g])
        datas = batch(r2[g].at[others], r2[g].at[others], send2.at[g], recv2.at[g])
        heads.wait_recv()
        datas.wait_recv()
        ends += [heads, datas]
        mine = here[STAGES[g][1]] * 4 + here[STAGES[g][2]]
        halves = []
        for half in range(2):
            row = jnp.zeros((1, CELL), F32)
            for n in range(8):
                source = cs2[g, mine, 0:1, :] if half + n == 0 else c2[g, half * 8 + n, 0:1, :]
                row = jnp.where(group_of == n, source, row)
            halves.append(row)
        scales = jnp.concatenate(halves, axis=1)
        rows = lax.broadcasted_iota(jnp.int32, (16, 256), 0)
        lanes = lax.broadcasted_iota(jnp.int32, (16, 256), 1) % 16
        select = jnp.where(rows == lanes, scales, 0.0).astype(BF16)
        for row in range(ROWS[g]):
            data = jnp.concatenate(
                [q2[g][mine, row]] + [r2[g][n, row] for n in range(1, 16)], axis=0
            )
            both = jnp.dot(select, decode(data), preferred_element_type=F32)
            final_ref[pl.ds((FIRST[g] + row) * TARGETS, TARGETS), :] = (
                both[:, :CELL] + both[:, CELL:]
            )
    for t in range(TARGETS):
        numer = final_ref[pl.ds(t, 12, stride=TARGETS), :]
        fraction = final_ref[pl.ds(12 * TARGETS + t, 1), :]
        filled = numer + jnp.maximum(0.25 - fraction, 0.0) * mean
        out_ref[:, t * CELL : (t + 1) * CELL] = filled / jnp.maximum(fraction, 0.25)
    for copy in ends:
        copy.wait_send()
    for g in range(3):
        mine = pl.ds(1, 7) if g else pl.ds(0, 7)
        batch(q[g].at[mine], q[g].at[mine], send1.at[g], recv1.at[g, 0]).wait_send()
        for half in range(2 if g else 1):
            heads = cs.at[half, g, mine]
            batch(heads, heads, csend.at[g, half], crecv.at[g, half]).wait_send()


def body(fields, land_mask, intersection, send_slot, target_block, live_blocks):
    smem = pl.BlockSpec(memory_space=pltpu.SMEM)
    hbm = pl.BlockSpec(memory_space=pl.ANY)
    dma = pltpu.SemaphoreType.DMA
    vmem = pltpu.VMEM
    i16 = jnp.int16
    i32 = jnp.int32
    return pl.pallas_call(
        kernel,
        in_specs=[smem] + [hbm] * 5,
        out_shape=pltpu.VMEM((12, TARGETS * CELL), F32),
        scratch_shapes=[vmem((1, BLOCKS), i32), vmem((1, BLOCKS), i32)]
        + [vmem((12, BLOCKS * CELL), BF16), vmem((BLOCKS, CELL), i32)]
        + [vmem((BLOCKS, CELL, CELL), BF16), vmem((BLOCKS + 1, 16, CELL), BF16)]
        + [vmem((1, 512), i32), pltpu.SMEM((1, 512), i32)]
        + [vmem((n, CELL), F32) for n in (576, 384, 384)] * 2
        + [vmem((8, 4, r, 16, CELL), i16) for r in ROWS] * 2
        + [vmem((2, 3, 8, 2, CELL), F32)] * 2
        + [vmem((r, 256, CELL), F32) for r in ROWS]
        + [vmem((16, r, 16, CELL), i16) for r in ROWS] * 2
        + [vmem((3, 16, 1, CELL), F32)] * 2
        + [vmem((16 * TARGETS, CELL), F32)]
        + [vmem((2, 1, CELL), F32), vmem((8, 1, CELL), F32), vmem((16, 1, CELL), F32)]
        + [dma((5,)), dma((WEIGHT_COPIES,))]
        + [dma((3,)), dma((3, 2)), dma((3, 2)), dma((3, 2))]
        + [dma((3,))] * 4
        + [dma((2,))] * 2,
        compiler_params=pltpu.CompilerParams(
            collective_id=0, has_side_effects=True, vmem_limit_bytes=62 * 1024 * 1024
        ),
        name="remap",
    )(
        live_blocks,
        send_slot.reshape(1, BLOCKS),
        target_block.reshape(1, BLOCKS),
        fields,
        land_mask.reshape(BLOCKS, CELL),
        intersection,
    )


def solution(mesh):
    axes = ("band", "sub")
    return jax.shard_map(
        body,
        mesh=mesh,
        in_specs=(P(None, axes), P(axes), P(axes, None, None), P(axes), P(axes), P(axes)),
        out_specs=P(None, axes),
        check_vma=False,
    )
```

```python
import jax
import jax.numpy as jnp
from jax import lax
from jax.experimental import pallas as pl
from jax.experimental.pallas import tpu as pltpu
from jax.sharding import PartitionSpec as P

CELL = 128
BLOCKS = 256
TARGETS = 16
CHUNK = 64
ROWS = (5, 4, 4)
FIRST = (0, 5, 9)
STAGES = ("zxy", "xyz", "yzx")
SLOTS = ("zxy", "xzy", "yzx")
MESH = pl.DeviceIdType.MESH
F32 = jnp.float32
BF16 = jnp.bfloat16
WEIGHT_COPIES = 1


def encode(tiles, write):
    top = jnp.abs(tiles[0])
    for tile in tiles[1:]:
        top = jnp.maximum(top, jnp.abs(tile))
    top = jnp.maximum(jnp.max(top, axis=1, keepdims=True), 1e-25)
    power = jnp.ceil(jnp.log2(top) + 0.02)
    down = jnp.exp2(-power)
    for row, tile in enumerate(tiles):
        small = tile * down
        code = small * lax.rsqrt(jnp.abs(small) + 1e-30) * 32768.0
        write(row, jnp.round(code).astype(jnp.int32).astype(jnp.int16))
    return jnp.exp2(power - 30.0)


def spread(scale, period, lane):
    lanes = lax.broadcasted_iota(jnp.int32, (16, CELL), 1) % period
    slots = lax.broadcasted_iota(jnp.int32, (16, CELL), 0) + lane
    return jnp.sum(jnp.where(lanes == slots, scale, 0.0), axis=0, keepdims=True)


def decode(codes):
    value = codes.astype(F32)
    value = value * jnp.abs(value)
    high = value.astype(BF16)
    return jnp.concatenate([high, (value - high.astype(F32)).astype(BF16)], axis=1)


def kernel(
    live_ref, slot_hbm, target_hbm, fields_hbm, mask_hbm, weights_hbm, out_ref,
    slot_ref, target_ref, fields_ref, mask_ref, weights_ref, stack_ref, index_vmem, index_smem,
    even_a, even_b, even_c, odd_a, odd_b, odd_c, q_a, q_b, q_c, r1_a, r1_b, r1_c, cs, c1,
    s2_a, s2_b, s2_c, q2_a, q2_b, q2_c, r2_a, r2_b, r2_c, cs2, c2, final_ref, t_send, t1, t2,
    load, wload, send1, recv1, csend, crecv, send2, recv2, c2send, c2recv, tsend, trecv,
):
    stages = ((even_a, even_b, even_c), (odd_a, odd_b, odd_c))
    q = (q_a, q_b, q_c)
    r1 = (r1_a, r1_b, r1_c)
    s2 = (s2_a, s2_b, s2_c)
    q2 = (q2_a, q2_b, q2_c)
    r2 = (r2_a, r2_b, r2_c)
    band = lax.axis_index("band")
    here = {
        "y": band // 8,
        "x": lax.rem(band // 2, 4),
        "c": lax.rem(band, 2),
        "z": lax.axis_index("sub"),
    }

    def peer(**shifts):
        at = {}
        for dim in "yxcz":
            at[dim] = here[dim]
            if dim in shifts:
                at[dim] = lax.rem(here[dim] + shifts[dim], 2 if dim == "c" else 4)
        return at, ((at["y"] * 4 + at["x"]) * 2 + at["c"], at["z"])

    def remote(src, dst, send, recv, device):
        return pltpu.make_async_remote_copy(
            src_ref=src, dst_ref=dst, send_sem=send, recv_sem=recv,
            device_id=device, device_id_type=MESH,
        )

    partner = peer(c=1)[1]

    def reach(t):
        near = 1 + 2 * here["c"]
        return jnp.where(t == 0, 2, jnp.where(t == 1, near, jnp.where(t == 2, 4 - near, 0)))

    loads = [
        pltpu.make_async_copy(slot_hbm, slot_ref, load.at[0]),
        pltpu.make_async_copy(target_hbm, target_ref, load.at[1]),
        pltpu.make_async_copy(mask_hbm, mask_ref, load.at[2]),
        pltpu.make_async_copy(fields_hbm, fields_ref, load.at[3]),
    ]
    size = BLOCKS // WEIGHT_COPIES
    weight_loads = [
        pltpu.make_async_copy(
            weights_hbm.at[pl.ds(i * size, size)], weights_ref.at[pl.ds(i * size, size)], wload.at[i]
        )
        for i in range(WEIGHT_COPIES)
    ]
    for copy in loads + weight_loads:
        copy.start()

    barrier = pltpu.get_barrier_semaphore()
    greeted = set()
    for g in range(3):
        for n in range(1, 8):
            greeted.add(tuple(sorted({STAGES[g][0]: n // 2, "c": n % 2}.items())))
    greeted = {tuple(item for item in names if item[1]) for names in greeted}
    for names in sorted(greeted):
        pl.semaphore_signal(
            barrier, inc=1, device_id=peer(**dict(names))[1], device_id_type=MESH
        )

    low = lax.broadcasted_iota(jnp.int32, (1, CELL), 1) < CHUNK
    blocks = lax.broadcasted_iota(jnp.int32, (8, BLOCKS), 1)
    kind = lax.broadcasted_iota(jnp.int32, (8, BLOCKS), 0)
    place = lax.broadcasted_iota(jnp.int32, (512, 1), 0)
    along = lax.broadcasted_iota(jnp.int32, (1, 512), 1)
    cs[...] = jnp.zeros_like(cs)
    loads[0].wait()
    loads[1].wait()
    facts = jnp.where(kind == 0, blocks - BLOCKS, jnp.broadcast_to(target_ref[...], (8, BLOCKS)))
    facts = facts.astype(F32).astype(BF16)
    index_copy = pltpu.make_async_copy(index_vmem, index_smem, load.at[4])

    def fill(g):
        order = SLOTS[g]

        def split(n):
            chunk, second, third, k = n // 64, (n // 16) % 4, (n // 4) % 4, n % 4
            if g == 0:
                first, core = reach(chunk // 2), 1 - chunk % 2
            else:
                first, core = chunk // 2, chunk % 2
                second = reach((second // 2 + core) % 2 * 2 + second % 2)
            at = {
                order[0]: (here[order[0]] + first) % 4,
                order[1]: (here[order[1]] + second) % 4,
                order[2]: (here[order[2]] + third) % 4,
                "c": (here["c"] + core) % 2,
            }
            return at, k

        at, k = split(place)
        wanted = (((at["y"] * 4 + at["x"]) * 2 + at["c"]) * 4 + at["z"]) * 4 + k
        hits = jnp.where(wanted == slot_ref[...], 1.0, 0.0).astype(BF16)
        found = lax.dot_general(
            facts, hits, (((1,), (1,)), ((), ())), preferred_element_type=F32
        )
        if g == 0:
            index_vmem[...] = (found[0:1] + BLOCKS).astype(jnp.int32)
            index_copy.start()
        at, k = split(along)
        owner = at[STAGES[g][1]] * 4 + at[STAGES[g][2]]
        code = found[1:2] + (owner * TARGETS).astype(F32)
        for pair in range(4):
            both = code[:, pair * CELL : (pair + 1) * CELL]
            rolled = pltpu.roll(both, CHUNK, 1)
            for half in range(2 if g else 1):
                cs[half, g, 2 * pair, 0:1, :] = jnp.where(low, both, rolled)
                cs[half, g, 2 * pair + 1, 0:1, :] = jnp.where(low, rolled, both)

    fill(0)

    loads[2].wait()
    loads[3].wait()
    live = live_ref[0]

    def build(i, total):
        for j in range(8):
            block = i * 8 + j
            alive = (block < live).astype(jnp.int32)
            mask = (mask_ref[pl.ds(block, 1), :] * alive).astype(F32)
            values = fields_ref[:, pl.ds(pl.multiple_of(block * CELL, CELL), CELL)].astype(F32)
            stacked = jnp.concatenate([values * mask, jnp.broadcast_to(mask, (4, CELL))], axis=0)
            total += stacked
            stack_ref[block] = stacked.astype(BF16)
        return total

    total = lax.fori_loop(0, BLOCKS // 8, build, jnp.zeros((16, CELL), F32))
    stack_ref[BLOCKS] = jnp.zeros((16, CELL), BF16)
    t_send[0] = spread(jnp.sum(total, axis=1, keepdims=True), CELL, 0)
    fill(1)
    fill(2)
    pl.semaphore_wait(barrier, len(greeted))

    for slot in range(1, 8):
        remote(
            t_send.at[0], t1.at[slot], tsend.at[0], trecv.at[0], peer(z=slot // 2, c=slot % 2)[1]
        ).start()
    index_copy.wait()
    for copy in weight_loads:
        copy.wait()

    def products(t, core, group):
        mine = t * 2 + 1 - core
        stage = stages[core]
        results = []
        for j in range(8):
            at = mine * CHUNK + group * 8 + j
            block = jnp.clip(index_smem[0, at], 0, BLOCKS)
            results.append(
                jnp.dot(
                    stack_ref[block],
                    weights_ref[jnp.minimum(block, BLOCKS - 1)],
                    preferred_element_type=F32,
                )
            )
        for j in range(8):
            i, n = group // 2, (group % 2) * 8 + j
            value = results[j]
            starts = (
                i * 16 + n,
                i * ROWS[1] * 16 + n,
                (n // 4) * ROWS[2] * 16 + i * 4 + n % 4,
            )
            for g in range(3):
                part = value[FIRST[g] : FIRST[g] + ROWS[g]]
                stage[g][pl.ds(starts[g], ROWS[g], stride=16 if g else 64), :] = part

    def code_tile(t, core, g, u, rows):
        stage = stages[core][g]
        if g == 0:
            mine = t * 2 + 1 - core
            scale = encode(
                [stage[r * 64 + u * 16 : r * 64 + u * 16 + 16, :] for r in range(ROWS[0])],
                lambda r, v: q_a.__setitem__((mine, u, r), v),
            )
            rows.append(spread(scale, CHUNK, u * 16))
        else:
            base = u * ROWS[g] * 16
            slot = u * 2 + core
            scale = encode(
                [stage[base + r * 16 : base + r * 16 + 16, :] for r in range(ROWS[g])],
                lambda r, v: q[g].__setitem__((slot, t, r), v),
            )
            half = t // 2
            lane = lax.rem(half + core, 2) * 32 + lax.rem(t, 2) * 16
            cs[half, g, slot, 1:2, :] += spread(scale, CHUNK, lane)

    def ship(t, core, rows, home):
        half = t // 2
        mine = t * 2 + 1 - core
        cs[0, 0, mine, 1:2, :] = (rows[0] + rows[1]) + (rows[2] + rows[3])
        if not home:
            device = peer(z=reach(t), c=core)[1]
            remote(
                cs.at[0, 0, mine], c1.at[0, 0, mine], csend.at[0, 0], crecv.at[0, half], device
            ).start()
            remote(q_a.at[mine], r1_a.at[mine], send1.at[0], recv1.at[0, half], device).start()
        for u in (2, 1, 3, 0):
            for g in (1, 2):
                if u or core:
                    slot = u * 2 + core
                    remote(
                        q[g].at[slot, t], r1[g].at[slot, t], send1.at[g], recv1.at[g, half],
                        peer(**{STAGES[g][0]: u, "c": core})[1],
                    ).start()

    def ship_heads(half):
        for slot in range(1, 8):
            for g in (1, 2):
                remote(
                    cs.at[half, g, slot], c1.at[half, g, slot],
                    csend.at[g, half], crecv.at[g, half],
                    peer(**{STAGES[g][0]: slot // 2, "c": slot % 2})[1],
                ).start()

    tiles = [(g, u) for g in range(3) for u in range(4)]

    def together(ahead, behind, home=False):
        rows = []
        done = 0
        for group in range(8):
            if ahead is not None:
                products(*ahead, group)
            if behind is not None:
                upto = (group + 1) * len(tiles) // 8
                for g, u in tiles[done:upto]:
                    code_tile(*behind, g, u, rows)
                done = upto
        if behind is not None:
            ship(*behind, rows, home)

    together((0, 1), None)

    def step(t, carry):
        together((t, 0), (t, 1))
        together((t + 1, 1), (t, 0))

        @pl.when(t == 1)
        def _():
            ship_heads(0)

        return carry

    lax.fori_loop(0, 3, step, 0)
    together((3, 0), (3, 1))
    together(None, (3, 0), home=True)

    ship_heads(1)

    def batch(src, dst, send, recv):
        return remote(src, dst, send, recv, partner)

    rest = pl.ds(1, 7)
    sums_first = batch(t1.at[rest], t1.at[rest], tsend.at[0], trecv.at[0])
    far = sorted(range(1, 16), key=lambda n: -(min(n // 4, 4 - n // 4) + min(n % 4, 4 - n % 4)))
    ends = [sums_first]
    others = pl.ds(1, 15)
    quarter = lax.broadcasted_iota(jnp.int32, (1, CELL), 1) // 32

    def combine(g, half):
        if g == 0:
            slots = list(range(4 * half, 4 * half + 4))
            n = 4 - half
            heads, datas = c1.at[0, 0, pl.ds(4 * half, n)], r1_a.at[pl.ds(4 * half, n)]
            pieces = [(slot, part) for slot in slots for part in range(4)]
            own = 7
        else:
            slots = [slot ^ half for slot in range(8)]
            heads = c1.at[half, g, rest]
            datas = r1[g].at[rest, pl.ds(2 * half, 2)]
            pieces = [(slot, 2 * half + part) for slot in slots for part in range(2)]
            own = 0
        batch(heads, heads, csend.at[g, 0], crecv.at[g, half]).wait_recv()
        batch(datas, datas, send1.at[g], recv1.at[g, half]).wait_recv()

        def lane_row(at):
            level = half if g else 0
            rows = [
                (cs if slot == own else c1)[level, g, slot, at : at + 1, :] for slot in slots
            ]
            if g == 0:
                parts = [jnp.where(low, rows[2 * p], rows[2 * p + 1]) for p in range(2)]
            else:
                parts = []
                for p in range(2):
                    a, b, c, d = rows[4 * p : 4 * p + 4]
                    parts.append(
                        jnp.where(low, jnp.where(quarter == 0, a, b), jnp.where(quarter == 2, c, d))
                    )
            return jnp.concatenate(parts, axis=1)

        targets = lax.broadcasted_iota(jnp.int32, (256, 256), 0).astype(F32)
        select = jnp.where(targets == lane_row(0), lane_row(1), 0.0).astype(BF16)
        for row in range(ROWS[g]):
            data = jnp.concatenate(
                [(q if slot == own else r1)[g][slot, part, row] for slot, part in pieces], axis=0
            )
            both = jnp.dot(select, decode(data), preferred_element_type=F32)
            both = both[:, :CELL] + both[:, CELL:]
            s2[g][row] = s2[g][row] + both if half else both

    for g in (1, 2, 0):
        if g == 0:
            sums_first.wait_recv()
            total = t_send[0]
            for slot in range(1, 8):
                total += t1[slot]
            t_send[1] = total
            for n in far:
                remote(
                    t_send.at[1], t2.at[n], tsend.at[1], trecv.at[1], peer(x=n // 4, y=n % 4)[1]
                ).start()
        for other in {1: (1, 2), 2: (), 0: (0,)}[g]:
            combine(other, 0)
        combine(g, 1)
        for owner in range(16):
            scale = encode(
                [s2[g][r, owner * 16 : owner * 16 + 16, :] for r in range(ROWS[g])],
                lambda r, v: q2[g].__setitem__((owner, r), v),
            )
            cs2[g, owner, 0:1, :] = spread(scale, 16, 0)
        second, third = STAGES[g][1:]
        for n in far:
            at, device = peer(**{second: n // 4, third: n % 4})
            owner = at[second] * 4 + at[third]
            remote(
                cs2.at[g, owner], c2.at[g, n], c2send.at[g], c2recv.at[g], device
            ).start()
        for n in far:
            at, device = peer(**{second: n // 4, third: n % 4})
            owner = at[second] * 4 + at[third]
            remote(q2[g].at[owner], r2[g].at[n], send2.at[g], recv2.at[g], device).start()

    sums_second = batch(t2.at[others], t2.at[others], tsend.at[1], trecv.at[1])
    sums_second.wait_recv()
    ends.append(sums_second)
    total = t_send[1]
    for n in range(1, 16):
        total += t2[n]
    lanes = lax.broadcasted_iota(jnp.int32, (16, CELL), 1)
    rows = lax.broadcasted_iota(jnp.int32, (16, CELL), 0)
    total = jnp.sum(jnp.where(lanes == rows, total, 0.0), axis=1, keepdims=True)
    mean = total[0:12] / jnp.maximum(total[12:13], 1.0)
    group_of = lax.broadcasted_iota(jnp.int32, (1, CELL), 1) // 16
    for g in (1, 2, 0):
        heads = batch(c2.at[g, others], c2.at[g, others], c2send.at[g], c2recv.at[g])
        datas = batch(r2[g].at[others], r2[g].at[others], send2.at[g], recv2.at[g])
        heads.wait_recv()
        datas.wait_recv()
        ends += [heads, datas]
        mine = here[STAGES[g][1]] * 4 + here[STAGES[g][2]]
        halves = []
        for half in range(2):
            row = jnp.zeros((1, CELL), F32)
            for n in range(8):
                source = cs2[g, mine, 0:1, :] if half + n == 0 else c2[g, half * 8 + n, 0:1, :]
                row = jnp.where(group_of == n, source, row)
            halves.append(row)
        scales = jnp.concatenate(halves, axis=1)
        rows = lax.broadcasted_iota(jnp.int32, (16, 256), 0)
        lanes = lax.broadcasted_iota(jnp.int32, (16, 256), 1) % 16
        select = jnp.where(rows == lanes, scales, 0.0).astype(BF16)
        for row in range(ROWS[g]):
            data = jnp.concatenate(
                [q2[g][mine, row]] + [r2[g][n, row] for n in range(1, 16)], axis=0
            )
            both = jnp.dot(select, decode(data), preferred_element_type=F32)
            final_ref[pl.ds((FIRST[g] + row) * TARGETS, TARGETS), :] = (
                both[:, :CELL] + both[:, CELL:]
            )
    for t in range(TARGETS):
        numer = final_ref[pl.ds(t, 12, stride=TARGETS), :]
        fraction = final_ref[pl.ds(12 * TARGETS + t, 1), :]
        filled = numer + jnp.maximum(0.25 - fraction, 0.0) * mean
        out_ref[:, t * CELL : (t + 1) * CELL] = filled / jnp.maximum(fraction, 0.25)
    for copy in ends:
        copy.wait_send()
    for g in range(3):
        mine = pl.ds(1, 7) if g else pl.ds(0, 7)
        batch(q[g].at[mine], q[g].at[mine], send1.at[g], recv1.at[g, 0]).wait_send()
        for half in range(2 if g else 1):
            heads = cs.at[half, g, mine]
            batch(heads, heads, csend.at[g, half], crecv.at[g, half]).wait_send()


def body(fields, land_mask, intersection, send_slot, target_block, live_blocks):
    smem = pl.BlockSpec(memory_space=pltpu.SMEM)
    hbm = pl.BlockSpec(memory_space=pl.ANY)
    dma = pltpu.SemaphoreType.DMA
    vmem = pltpu.VMEM
    i16 = jnp.int16
    i32 = jnp.int32
    return pl.pallas_call(
        kernel,
        in_specs=[smem] + [hbm] * 5,
        out_shape=pltpu.VMEM((12, TARGETS * CELL), F32),
        scratch_shapes=[vmem((1, BLOCKS), i32), vmem((1, BLOCKS), i32)]
        + [vmem((12, BLOCKS * CELL), BF16), vmem((BLOCKS, CELL), i32)]
        + [vmem((BLOCKS, CELL, CELL), BF16), vmem((BLOCKS + 1, 16, CELL), BF16)]
        + [vmem((1, 512), i32), pltpu.SMEM((1, 512), i32)]
        + [vmem((n, CELL), F32) for n in (576, 384, 384)] * 2
        + [vmem((8, 4, r, 16, CELL), i16) for r in ROWS] * 2
        + [vmem((2, 3, 8, 2, CELL), F32)] * 2
        + [vmem((r, 256, CELL), F32) for r in ROWS]
        + [vmem((16, r, 16, CELL), i16) for r in ROWS] * 2
        + [vmem((3, 16, 1, CELL), F32)] * 2
        + [vmem((16 * TARGETS, CELL), F32)]
        + [vmem((2, 1, CELL), F32), vmem((8, 1, CELL), F32), vmem((16, 1, CELL), F32)]
        + [dma((5,)), dma((WEIGHT_COPIES,))]
        + [dma((3,)), dma((3, 2)), dma((3, 2)), dma((3, 2))]
        + [dma((3,))] * 4
        + [dma((2,))] * 2,
        compiler_params=pltpu.CompilerParams(
            collective_id=0, has_side_effects=True, vmem_limit_bytes=62 * 1024 * 1024
        ),
        name="remap",
    )(
        live_blocks,
        send_slot.reshape(1, BLOCKS),
        target_block.reshape(1, BLOCKS),
        fields,
        land_mask.reshape(BLOCKS, CELL),
        intersection,
    )


def solution(mesh):
    axes = ("band", "sub")
    return jax.shard_map(
        body,
        mesh=mesh,
        in_specs=(P(None, axes), P(axes), P(axes, None, None), P(axes), P(axes), P(axes)),
        out_specs=P(None, axes),
        check_vma=False,
    )
```
